16 devices in a mesh: dp: 2 (over y, z), cp: 8 (over x, core).
Axes of the slice: x: 4, y: 2, z: 1, core: 2. Of those that a mesh axis runs over, the one named last changes fastest.
The devices are a block of a 4x4x8 slice.
Arguments:
- queries: bfloat16 [4, 1024, 16, 128], P('dp', 'cp'), parts along dimension 0
- key_states: bfloat16 [4, 1024, 128], P('dp', 'cp'), parts along dimension 0
- value_states: bfloat16 [4, 1024, 128], P('dp', 'cp'), parts along dimension 0
- segment_ids: int32 [4, 1024], P('dp', 'cp'), parts along dimension 0
Outputs:
- output 1: bfloat16 [4, 1024, 16, 128], P('dp', 'cp'), parts along dimension 0
- output 2: float32 [4, 1024, 16], P('dp', 'cp'), parts along dimension 0
There are 2 independent parts. The reference program is written for one: setup_inputs(seed, part) draws one part's arguments, and reference() takes and returns one part's arrays. A program takes and returns all parts, laid end to end along the dimension named above; each array names one.
All inputs are finite; a program needn't handle non-finite values.
Results may differ from the reference program's by a relative error of at most 0.00303282.
Values are sent between devices in bfloat16 or wider.
A program may use at most 768 MiB of HBM per device.

```python
import jax
import jax.numpy as jnp
from jax import lax

BATCH = 2
SEQ = 1024
HEADS = 16
HEAD = 128
CUTS = 2
QUERY_BLOCK = 64


def setup_inputs(seed: int = 0, part: int = 0) -> dict:
    base_key = jax.random.fold_in(jax.random.key(seed), part)
    sub_keys = jax.random.split(base_key, 5)
    queries = jax.random.normal(sub_keys[0], (BATCH, SEQ, HEADS, HEAD), jnp.float32)
    key_states = jax.random.normal(sub_keys[1], (BATCH, SEQ, HEAD), jnp.float32)
    value_noise = jax.random.normal(sub_keys[2], (BATCH, SEQ, HEAD), jnp.float32)
    drift = jnp.cumsum(jax.random.normal(sub_keys[3], (BATCH, SEQ, HEAD), jnp.float32), axis=1) * (2.0 / SEQ) ** 0.5
    value_states = 0.5 * value_noise + drift
    cut_points = jax.random.randint(sub_keys[4], (BATCH, CUTS), 1, SEQ)
    positions = jnp.arange(SEQ)
    segment_ids = jnp.sum((positions[None, :, None] >= cut_points[:, None, :]).astype(jnp.int32), axis=-1)
    return {
        "queries": queries.astype(jnp.bfloat16),
        "key_states": key_states.astype(jnp.bfloat16),
        "value_states": value_states.astype(jnp.bfloat16),
        "segment_ids": segment_ids.astype(jnp.int32),
    }


def reference(queries, key_states, value_states, segment_ids):
    score_scale = HEAD ** -0.5
    num_blocks = SEQ // QUERY_BLOCK
    key_pos = jnp.arange(SEQ)

    def one_row(row_inputs):
        q_row, k_row, v_row, seg_row = row_inputs
        k_wide = k_row.astype(jnp.float32)
        v_wide = v_row.astype(jnp.float32)

        def one_block(blk_idx):
            row_start = blk_idx * QUERY_BLOCK
            q_blk = lax.dynamic_slice_in_dim(q_row, row_start, QUERY_BLOCK, 0).astype(jnp.float32)
            seg_blk = lax.dynamic_slice_in_dim(seg_row, row_start, QUERY_BLOCK, 0)
            q_pos = row_start + jnp.arange(QUERY_BLOCK)
            visible = (key_pos[None, :] <= q_pos[:, None]) & (seg_row[None, :] == seg_blk[:, None])
            scores = jnp.einsum("qhd,kd->qhk", q_blk, k_wide) * score_scale
            scores = jnp.where(visible[:, None, :], scores, -jnp.inf)
            row_max = jnp.max(scores, axis=-1)
            weights = jnp.exp(scores - row_max[..., None])
            weight_sum = jnp.sum(weights, axis=-1)
            weighted = jnp.einsum("qhk,kd->qhd", weights, v_wide) / weight_sum[..., None]
            return weighted.astype(jnp.bfloat16), row_max + jnp.log(weight_sum)

        out_blocks, lse_blocks = lax.map(one_block, jnp.arange(num_blocks))
        return out_blocks.reshape(SEQ, HEADS, HEAD), lse_blocks.reshape(SEQ, HEADS)

    attn_out, log_sum_exp = lax.map(one_row, (queries, key_states, value_states, segment_ids))
    return attn_out, log_sum_exp
```

```python
import jax
import jax.numpy as jnp
import numpy as np
from jax import lax
from jax.experimental import pallas as pl
from jax.experimental.pallas import tpu as pltpu
from jax.sharding import PartitionSpec as P

MESH = pl.DeviceIdType.MESH
F32, BF16 = jnp.float32, jnp.bfloat16
HIDE = float(jnp.finfo(jnp.bfloat16).min)
LN2 = float(np.log(2.0))
LOG2E = float(np.log2(np.e))
NEXT, PREV, PART = 0, 1, 2
K, V, SEG = 0, 1, 2

ORDER = {
    0: [(0, 0), (0, 1)],
    1: [(1, 0), (1, 1), (0, 0), (0, 1)],
    2: [(2, 0), (2, 1), (1, 0), (1, 1), (0, 0), (0, 1)],
    3: [(3, 0), (3, 1), (2, 0), (0, 0), (2, 1), (0, 1), (1, 0), (1, 1)],
}


def pieces(c, q, b):
    return ([(SEG, c, q, 0)] if b == 0 else []) + [(K, c, q, b), (V, c, q, b)]


def unit(c, b):
    return pieces(c, 1, b) + pieces(c, 0, b)


def schedule():
    plan = {(c, q): {} for c in range(4) for q in range(2)}

    def put(c, q, step, *acts):
        plan[c, q].setdefault(step, []).extend(acts)

    def send(items, *ways):
        return [("send", i, w) for i in items for w in ways]

    def take(items, *ways):
        return [a for i in items for a in [("wait", i)] + [("send", i, w) for w in ways]]

    for c in range(4):
        put(c, 0, 0, *send(pieces(c, 0, 0) + pieces(c, 0, 1), PART))
        for s, (uc, b) in enumerate(ORDER[c]):
            put(c, 0, s, *take(pieces(c, 1, b) if uc == c else unit(uc, b)))
    own = lambda c: pieces(c, 1, 0) + pieces(c, 1, 1)
    put(0, 1, 0, *send(own(0), NEXT, PREV), *send(own(0), PART))
    put(0, 1, 0, *take(pieces(0, 0, 0) + pieces(0, 0, 1), NEXT, PREV))
    put(0, 1, 0, *take(pieces(1, 1, 1) + pieces(1, 0, 1), PREV))
    put(1, 1, 0, *send(own(1), NEXT), *send(pieces(1, 1, 1), PREV), *send(own(1), PART))
    put(1, 1, 0, *take(pieces(1, 0, 0), NEXT), *take(pieces(1, 0, 1), NEXT, PREV))
    put(1, 1, 1, *take(pieces(0, 1, 0), NEXT, PART))
    put(1, 1, 2, *take(pieces(0, 0, 0), NEXT, PART), *take(unit(0, 1), PART))
    put(2, 1, 0, *send(own(2), NEXT), *send(own(2), PART))
    put(2, 1, 0, *take(pieces(2, 0, 0) + pieces(2, 0, 1), NEXT))
    put(2, 1, 1, *take(pieces(1, 1, 0), NEXT, PART))
    put(2, 1, 2, *take(pieces(1, 0, 0), NEXT, PART))
    put(2, 1, 3, *take(unit(1, 1), PART))
    put(2, 1, 4, *take(unit(0, 0), PART))
    put(2, 1, 5, *take(unit(0, 1), PART))
    put(3, 1, 0, *send(own(3), PART), *take(pieces(3, 0, 0)))
    put(3, 1, 1, *take(pieces(3, 0, 1)), *take(pieces(2, 1, 0), PART))
    put(3, 1, 2, *take(pieces(2, 0, 0), PART))
    put(3, 1, 3, *take(unit(0, 0), PART))
    put(3, 1, 4, *take(unit(2, 1), PART))
    put(3, 1, 5, *take(unit(0, 1), PART, PREV))
    put(3, 1, 6, *take(unit(1, 0), PART))
    put(3, 1, 7, *take(unit(1, 1), PART))
    return plan


PLAN = schedule()


def attend(lhs, kk, vv, m_ref, l_ref, acc_ref, b, scale):
    s = lax.dot_general(lhs, kk, (((1,), (1,)), ((), ())), preferred_element_type=F32) * scale
    m_prev = m_ref[b]
    m_new = jnp.maximum(m_prev, jnp.max(jnp.maximum(s[:, :128], s[:, 128:]), axis=1, keepdims=True))
    p0 = jnp.exp2(s[:, :128] - m_new)
    p1 = jnp.exp2(s[:, 128:] - m_new)
    alpha = jnp.exp2(m_prev - m_new)
    m_ref[b] = m_new
    l_ref[b] = l_ref[b] * alpha + (p0 + p1)
    p = jnp.concatenate([p0.astype(BF16), p1.astype(BF16)], axis=1)
    pv = lax.dot_general(p, vv, (((1,), (0,)), ((), ())), preferred_element_type=F32)
    acc_ref[b] = acc_ref[b] * alpha + pv


def kernel(q_hbm, k_hbm, v_hbm, seg_hbm, o_ref, lse_ref, qb, oh, kb, vb, sg, m_ref, l_ref, acc_ref, qsem, ldsem, sgsem, ssem, rsem, sssem, srsem):
    me = lax.axis_index("cp")
    chip, core = me // 2, me % 2
    rows = qb.shape[1]
    heads = rows // 128
    scale = 128**-0.5 * LOG2E

    def slot(item):
        kind, c, q, b = item
        if kind == SEG:
            return sg.at[c * 2 + q]
        return (kb, vb)[kind].at[c, b, pl.ds(q * 128, 128), :]

    loads = {SEG: pltpu.make_async_copy(seg_hbm, sg.at[me], sgsem)}
    for kind, src in ((K, k_hbm), (V, v_hbm)):
        for b in range(2):
            loads[kind, b] = pltpu.make_async_copy(src.at[b], (kb, vb)[kind].at[chip, b, pl.ds(core * 128, 128), :], ldsem.at[kind, b])
    for copy in loads.values():
        copy.start()
    q_loads = [pltpu.make_async_copy(q_hbm.at[b], qb.at[b], qsem.at[b]) for b in range(2)]
    for copy in q_loads:
        copy.start()

    barrier = pltpu.get_barrier_semaphore()
    next_dev = lax.rem(chip + 1, 4) * 2 + 1
    prev_dev = lax.rem(chip + 3, 4) * 2 + 1
    part_dev = chip * 2 + 1 - core
    pl.semaphore_signal(barrier, inc=1, device_id={"cp": part_dev}, device_id_type=MESH)

    @pl.when(core == 1)
    def _():
        for dev in (next_dev, prev_dev):
            pl.semaphore_signal(barrier, inc=1, device_id={"cp": dev}, device_id_type=MESH)
        pl.semaphore_wait(barrier, 3)

    @pl.when(core == 0)
    def _():
        pl.semaphore_wait(barrier, 1)

    ways = (next_dev, prev_dev, part_dev)

    def remote(item, way):
        kind, c, q, b = item
        sems = (sssem.at[way, c * 2 + q], srsem.at[c * 2 + q]) if kind == SEG else (ssem.at[way, kind, c, q, b], rsem.at[kind, c, q, b])
        ref = slot(item)
        return pltpu.make_async_remote_copy(src_ref=ref, dst_ref=ref, send_sem=sems[0], recv_sem=sems[1], device_id={"cp": ways[way]}, device_id_type=MESH)

    def run(actions):
        for act in actions:
            if act[0] == "wait":
                remote(act[1], PART).wait_recv()
            else:
                remote(act[1], act[2]).start()

    for copy in loads.values():
        copy.wait()
    for (c, q), steps in PLAN.items():
        pl.when((chip == c) & (core == q))(lambda a=steps[0]: run(a))

    def fill(t, _):
        here = lax.broadcasted_iota(jnp.int32, (heads, 128), 1) == t
        oh[pl.ds(pl.multiple_of(t * heads, heads), heads), :] = jnp.where(here, 1.0, 0.0).astype(BF16)
        return 0

    lax.fori_loop(0, 128, fill, 0, unroll=8)
    m_ref[...] = jnp.full(m_ref.shape, HIDE, F32)
    l_ref[...] = jnp.zeros(l_ref.shape, F32)
    acc_ref[...] = jnp.zeros(acc_ref.shape, F32)
    for copy in q_loads:
        copy.wait()

    def pack(units):
        return sum((c * 2 + b) * 8**i for i, (c, b) in enumerate(units))

    todo0 = jnp.where(chip == 0, pack(ORDER[0]), jnp.where(chip == 1, pack(ORDER[1]), jnp.where(chip == 2, pack(ORDER[2]), pack(ORDER[3]))))

    def step(s, todo):
        code = todo % 8
        c, b = code // 2, code % 2

        @pl.when(s > 0)
        def _():
            for cc in range(4):
                for qq in range(2):
                    acts = {i: a for i, a in PLAN[cc, qq].items() if i > 0}

                    @pl.when((chip == cc) & (core == qq))
                    def _(acts=acts):
                        for i, a in acts.items():
                            pl.when(s == i)(lambda a=a: run(a))

        seg_t = sg[me, pl.ds(b, 1), :].astype(F32)
        bias = []
        for half in range(2):
            seg_u = sg[c * 2 + half, pl.ds(b, 1), :].astype(F32)
            seg_u = jnp.broadcast_to(seg_u, (128, 128)).T
            u_pos = c * 256 + half * 128 + lax.broadcasted_iota(jnp.int32, (128, 128), 0)
            t_pos = me * 128 + lax.broadcasted_iota(jnp.int32, (128, 128), 1)
            bias.append(jnp.where((seg_u == seg_t) & (u_pos <= t_pos), 0.0, HIDE).astype(BF16))
        kk = jnp.concatenate([kb[c, b], jnp.concatenate(bias, axis=0)], axis=1)
        lhs = jnp.concatenate([qb[b], oh[...]], axis=1)
        attend(lhs, kk, vb[c, b], m_ref, l_ref, acc_ref, b, scale)
        return todo // 8

    lax.fori_loop(0, 2 * (chip + 1), step, todo0)

    head_lane = lax.broadcasted_iota(jnp.int32, (128, heads, 128), 2) == lax.broadcasted_iota(jnp.int32, (128, heads, 128), 1)
    for b in range(2):
        total = jnp.sum(l_ref[b], axis=1, keepdims=True)
        o_ref[b] = (acc_ref[b] / total).astype(BF16)
        lse = (m_ref[b] * LN2 + jnp.log(total)).reshape(128, heads, 128)
        lse_ref[b] = jnp.sum(jnp.where(head_lane, lse, 0.0), axis=1).T[:heads, :]

    for (c, q), steps in PLAN.items():

        @pl.when((chip == c) & (core == q))
        def _(steps=steps):
            for acts in steps.values():
                for act in acts:
                    if act[0] == "send":
                        remote(act[1], act[2]).wait_send()


def solution(mesh):
    def local(q, k, v, seg):
        batch, seq, heads, head = q.shape
        rows = seq * heads
        out, lse = pl.pallas_call(
            kernel,
            out_shape=(pltpu.VMEM((batch, rows, head), BF16), pltpu.VMEM((batch, heads, seq), F32)),
            in_specs=[pl.BlockSpec(memory_space=pltpu.HBM)] * 4,
            out_specs=(pl.BlockSpec(memory_space=pltpu.VMEM),) * 2,
            scratch_shapes=[
                pltpu.VMEM((batch, rows, head), BF16),
                pltpu.VMEM((rows, 128), BF16),
                pltpu.VMEM((4, batch, 2 * seq, head), BF16),
                pltpu.VMEM((4, batch, 2 * seq, head), BF16),
                pltpu.VMEM((8, batch, seq), jnp.int32),
                pltpu.VMEM((batch, rows, 128), F32),
                pltpu.VMEM((batch, rows, 128), F32),
                pltpu.VMEM((batch, rows, 128), F32),
                pltpu.SemaphoreType.DMA((2,)),
                pltpu.SemaphoreType.DMA((2, 2)),
                pltpu.SemaphoreType.DMA,
                pltpu.SemaphoreType.DMA((3, 2, 4, 2, 2)),
                pltpu.SemaphoreType.DMA((2, 4, 2, 2)),
                pltpu.SemaphoreType.DMA((3, 8)),
                pltpu.SemaphoreType.DMA((8,)),
            ],
            compiler_params=pltpu.CompilerParams(collective_id=0, has_side_effects=True, vmem_limit_bytes=48 * 2**20),
        )(q.reshape(batch, rows, head), k, v, seg)
        return out.reshape(q.shape), lse.transpose(0, 2, 1)

    return jax.shard_map(
        local,
        mesh=mesh,
        in_specs=(P("dp", "cp", None, None), P("dp", "cp", None), P("dp", "cp", None), P("dp", "cp")),
        out_specs=(P("dp", "cp", None, None), P("dp", "cp", None)),
        check_vma=False,
    )
```

```python
import jax
import jax.numpy as jnp
import numpy as np
from jax import lax
from jax.experimental import pallas as pl
from jax.experimental.pallas import tpu as pltpu
from jax.sharding import PartitionSpec as P

MESH = pl.DeviceIdType.MESH
F32, BF16 = jnp.float32, jnp.bfloat16
HIDE = float(jnp.finfo(jnp.bfloat16).min)
LOG2E = float(np.log2(np.e))
NEXT, PREV, PART = 0, 1, 2
K, V, SEG = 0, 1, 2

ORDER = {
    0: [],
    1: [(0, 0), (0, 1)],
    2: [(1, 0), (1, 1), (0, 0), (0, 1)],
    3: [(2, 0), (0, 0), (2, 1), (0, 1), (1, 0), (1, 1)],
}


def pieces(c, q, b):
    return ([(SEG, c, q, 0)] if b == 0 else []) + [(K, c, q, b), (V, c, q, b)]


def unit(c, b):
    return pieces(c, 1, b) + pieces(c, 0, b)


def schedule():
    plan = {(c, q): {} for c in range(4) for q in range(2)}

    def put(c, q, step, *acts):
        plan[c, q].setdefault(step, []).extend(acts)

    def send(items, *ways):
        return [("send", i, w) for i in items for w in ways]

    def take(items, *ways):
        return [a for i in items for a in [("wait", i)] + [("send", i, w) for w in ways]]

    for c in range(4):
        put(c, 0, 0, *send(pieces(c, 0, 0) + pieces(c, 0, 1), PART))
        put(c, 0, 1, *take(pieces(c, 1, 0) + pieces(c, 1, 1)))
    own = lambda c: pieces(c, 1, 0) + pieces(c, 1, 1)
    put(0, 1, 0, *send(own(0), NEXT, PREV), *send(own(0), PART))
    put(0, 1, 1, *take(pieces(0, 0, 0) + pieces(0, 0, 1), NEXT, PREV))
    put(0, 1, 1, *take(pieces(1, 1, 1) + pieces(1, 0, 1), PREV))
    put(1, 1, 0, *send(own(1), NEXT), *send(pieces(1, 1, 1), PREV), *send(own(1), PART))
    put(1, 1, 1, *take(pieces(1, 0, 0), NEXT), *take(pieces(1, 0, 1), NEXT, PREV))
    put(1, 1, 2, *take(unit(0, 0), NEXT, PART))
    put(1, 1, 3, *take(unit(0, 1), PART))
    put(2, 1, 0, *send(own(2), NEXT), *send(own(2), PART))
    put(2, 1, 1, *take(pieces(2, 0, 0) + pieces(2, 0, 1), NEXT))
    put(2, 1, 2, *take(unit(1, 0), NEXT, PART))
    put(2, 1, 3, *take(unit(1, 1), PART))
    put(2, 1, 4, *take(unit(0, 0), PART))
    put(2, 1, 5, *take(unit(0, 1), PART))
    put(3, 1, 0, *send(own(3), PART))
    put(3, 1, 1, *take(pieces(3, 0, 0)), *take(pieces(3, 0, 1)))
    put(3, 1, 2, *take(unit(2, 0), PART))
    put(3, 1, 3, *take(unit(0, 0), PART))
    put(3, 1, 4, *take(unit(2, 1), PART))
    put(3, 1, 5, *take(unit(0, 1), PART, PREV))
    put(3, 1, 6, *take(unit(1, 0), PART))
    put(3, 1, 7, *take(unit(1, 1), PART))
    return plan


PLAN = schedule()


def attend(lhs, kk, vv, state, b, c2, first=False):
    m_ref, l_ref, acc_ref = state
    s = lax.dot_general(lhs, kk, (((1,), (1,)), ((), ())), preferred_element_type=F32)
    m_new = jnp.broadcast_to(jnp.max(jnp.maximum(s[:, :128], s[:, 128:]), axis=1, keepdims=True), (s.shape[0], 128))
    if not first:
        m_prev = m_ref[b]
        m_new = jnp.maximum(m_prev, m_new)
        alpha = jnp.exp2((m_prev - m_new) * c2)
    p0 = jnp.exp2((s[:, :128] - m_new) * c2)
    p1 = jnp.exp2((s[:, 128:] - m_new) * c2)
    m_ref[b] = m_new
    p = jnp.concatenate([p0.astype(BF16), p1.astype(BF16)], axis=1)
    pv = lax.dot_general(p, vv, (((1,), (0,)), ((), ())), preferred_element_type=F32)
    l_ref[b] = p0 + p1 if first else l_ref[b] * alpha + (p0 + p1)
    acc_ref[b] = pv if first else acc_ref[b] * alpha + pv


def branch(index, leaves):
    keys = sorted(leaves)
    if len(keys) == 1:
        pl.when(index == keys[0])(leaves[keys[0]])
        return
    mid = keys[len(keys) // 2]
    pl.when(index < mid)(lambda: branch(index, {k: leaves[k] for k in keys if k < mid}))
    pl.when(index >= mid)(lambda: branch(index, {k: leaves[k] for k in keys if k >= mid}))


def kernel(q_hbm, k_hbm, v_hbm, seg_hbm, o_ref, lse_ref, qb, oh, kb, vb, sg, bias, m_ref, l_ref, acc_ref, qsem, ldsem, sgsem, ssem, rsem, sssem, srsem):
    me = lax.axis_index("cp")
    chip, core = me // 2, me % 2
    rows = qb.shape[1]
    heads = rows // 128
    scale = 128**-0.5
    c2 = scale * LOG2E

    def slot(item):
        kind, c, q, b = item
        if kind == SEG:
            return sg.at[c * 2 + q]
        return (kb, vb)[kind].at[c, b, pl.ds(q * 128, 128), :]

    loads = {SEG: pltpu.make_async_copy(seg_hbm, sg.at[me], sgsem)}
    for kind, src in ((K, k_hbm), (V, v_hbm)):
        for b in range(2):
            loads[kind, b] = pltpu.make_async_copy(src.at[b], (kb, vb)[kind].at[chip, b, pl.ds(core * 128, 128), :], ldsem.at[kind, b])
    for copy in loads.values():
        copy.start()
    q_loads = [pltpu.make_async_copy(q_hbm.at[b], qb.at[b], qsem.at[b]) for b in range(2)]
    for copy in q_loads:
        copy.start()

    barrier = pltpu.get_barrier_semaphore()
    next_dev = lax.rem(chip + 1, 4) * 2 + 1
    prev_dev = lax.rem(chip + 3, 4) * 2 + 1
    part_dev = chip * 2 + 1 - core
    pl.semaphore_signal(barrier, inc=1, device_id={"cp": part_dev}, device_id_type=MESH)

    @pl.when(core == 1)
    def _():
        for dev in (next_dev, prev_dev):
            pl.semaphore_signal(barrier, inc=1, device_id={"cp": dev}, device_id_type=MESH)
        pl.semaphore_wait(barrier, 3)

    @pl.when(core == 0)
    def _():
        pl.semaphore_wait(barrier, 1)

    ways = (next_dev, prev_dev, part_dev)

    def remote(item, way):
        kind, c, q, b = item
        sems = (sssem.at[way, c * 2 + q], srsem.at[c * 2 + q]) if kind == SEG else (ssem.at[way, kind, c, q, b], rsem.at[kind, c, q, b])
        ref = slot(item)
        return pltpu.make_async_remote_copy(src_ref=ref, dst_ref=ref, send_sem=sems[0], recv_sem=sems[1], device_id={"cp": ways[way]}, device_id_type=MESH)

    def run(actions):
        for act in actions:
            if act[0] == "wait":
                remote(act[1], PART).wait_recv()
            else:
                remote(act[1], act[2]).start()

    for copy in loads.values():
        copy.wait()
    branch(me, {c * 2 + q: lambda a=steps[0]: run(a) for (c, q), steps in PLAN.items()})

    def fill(t, _):
        here = lax.broadcasted_iota(jnp.int32, (heads, 128), 1) == t
        oh[pl.ds(pl.multiple_of(t * heads, heads), heads), :] = jnp.where(here, 1.0, 0.0).astype(BF16)
        return 0

    lax.fori_loop(0, 128, fill, 0, unroll=16)
    for copy in q_loads:
        copy.wait()

    def hide(c, b, buf, local=False):
        seg_t = sg[me, pl.ds(b, 1), :].astype(F32)
        for half in range(2):
            seg_u = sg[c * 2 + half, pl.ds(b, 1), :].astype(F32)
            seen = jnp.broadcast_to(seg_u, (128, 128)).T == seg_t
            if local:
                u_pos = half * 128 + lax.broadcasted_iota(jnp.int32, (128, 128), 0)
                t_pos = core * 128 + lax.broadcasted_iota(jnp.int32, (128, 128), 1)
                seen = seen & (u_pos <= t_pos)
            buf[pl.ds(half * 128, 128), :] = jnp.where(seen, 0.0, HIDE).astype(BF16)

    state = (m_ref, l_ref, acc_ref)

    def lhs(b):
        return jnp.concatenate([qb[b], oh[...]], axis=1)

    branch(me, {c * 2 + q: lambda a=steps[1]: run(a) for (c, q), steps in PLAN.items()})
    for b in range(2):
        hide(chip, b, bias.at[b], local=True)
    for b in range(2):
        kk = jnp.concatenate([kb[chip, b], bias[b]], axis=1)
        attend(lhs(b), kk, vb[chip, b], state, b, c2, first=True)

    def pack(units):
        return sum((c * 2 + b) * 8**i for i, (c, b) in enumerate(units))

    todo = jnp.where(chip == 1, pack(ORDER[1]), jnp.where(chip == 2, pack(ORDER[2]), pack(ORDER[3])))

    def step(s, todo):
        code = todo % 8
        c, b = code // 2, code % 2

        @pl.when(core == 1)
        def _():
            branch(chip, {cc: lambda acts={i: a for i, a in PLAN[cc, 1].items() if i > 1}: branch(s, {i: lambda a=a: run(a) for i, a in acts.items()}) for cc in (1, 2, 3)})

        @pl.when(core == 0)
        def _():
            @pl.when(b == 0)
            def _():
                for q in range(2):
                    remote((SEG, c, q, 0), PART).wait_recv()

            for q in (1, 0):
                for kind in (K, V):
                    remote((kind, c, q, b), PART).wait_recv()

        hide(c, b, bias.at[0])
        kk = jnp.concatenate([kb[c, b], bias[0]], axis=1)
        attend(lhs(b), kk, vb[c, b], state, b, c2)
        return todo // 8

    lax.fori_loop(2, 2 * (chip + 1), step, todo)

    lane = lax.broadcasted_iota(jnp.int32, (heads, 128), 1)
    for b in range(2):
        total = jnp.broadcast_to(jnp.sum(l_ref[b], axis=1, keepdims=True), (rows, 128))
        o_ref[b] = (acc_ref[b] * (1.0 / total)).astype(BF16)
        top, tot = m_ref[b, :heads, :], total[:heads]
        for t in range(1, 128):
            here = lane == t
            top = jnp.where(here, m_ref[b, t * heads : (t + 1) * heads, :], top)
            tot = jnp.where(here, total[t * heads : (t + 1) * heads], tot)
        lse_ref[b] = top * scale + jnp.log(tot)

    def drain(steps):
        for acts in steps.values():
            for act in acts:
                if act[0] == "send":
                    remote(act[1], act[2]).wait_send()

    branch(me, {c * 2 + q: lambda steps=steps: drain(steps) for (c, q), steps in PLAN.items()})


def solution(mesh):
    def local(q, k, v, seg):
        batch, seq, heads, head = q.shape
        rows = seq * heads
        out, lse = pl.pallas_call(
            kernel,
            out_shape=(pltpu.VMEM((batch, rows, head), BF16), pltpu.VMEM((batch, heads, seq), F32)),
            in_specs=[pl.BlockSpec(memory_space=pltpu.HBM)] * 4,
            out_specs=(pl.BlockSpec(memory_space=pltpu.VMEM),) * 2,
            scratch_shapes=[
                pltpu.VMEM((batch, rows, head), BF16),
                pltpu.VMEM((rows, 128), BF16),
                pltpu.VMEM((4, batch, 2 * seq, head), BF16),
                pltpu.VMEM((4, batch, 2 * seq, head), BF16),
                pltpu.VMEM((8, batch, seq), jnp.int32),
                pltpu.VMEM((2, 2 * seq, 128), BF16),
                pltpu.VMEM((batch, rows, 128), F32),
                pltpu.VMEM((batch, rows, 128), F32),
                pltpu.VMEM((batch, rows, 128), F32),
                pltpu.SemaphoreType.DMA((2,)),
                pltpu.SemaphoreType.DMA((2, 2)),
                pltpu.SemaphoreType.DMA,
                pltpu.SemaphoreType.DMA((3, 2, 4, 2, 2)),
                pltpu.SemaphoreType.DMA((2, 4, 2, 2)),
                pltpu.SemaphoreType.DMA((3, 8)),
                pltpu.SemaphoreType.DMA((8,)),
            ],
            compiler_params=pltpu.CompilerParams(collective_id=0, has_side_effects=True, vmem_limit_bytes=48 * 2**20),
        )(*[pltpu.with_memory_space_constraint(x, pltpu.HBM) for x in (q.reshape(batch, rows, head), k, v, seg)])
        return out.reshape(q.shape), lse.transpose(0, 2, 1)

    return jax.shard_map(
        local,
        mesh=mesh,
        in_specs=(P("dp", "cp", None, None), P("dp", "cp", None), P("dp", "cp", None), P("dp", "cp")),
        out_specs=(P("dp", "cp", None, None), P("dp", "cp", None)),
        check_vma=False,
    )
```

```python
import jax
import jax.numpy as jnp
import numpy as np
from jax import lax
from jax.experimental import pallas as pl
from jax.experimental.pallas import tpu as pltpu
from jax.sharding import PartitionSpec as P

MESH = pl.DeviceIdType.MESH
F32, BF16 = jnp.float32, jnp.bfloat16
HIDE = float(jnp.finfo(jnp.bfloat16).min)
LOG2E = float(np.log2(np.e))
NEXT, PREV, PART = 0, 1, 2
CHUNKS = 4
KV, SEG = 0, 1

ORDER = {
    0: [],
    1: [(0, 0), (0, 1)],
    2: [(1, 0), (1, 1), (0, 0), (0, 1)],
    3: [(2, 0), (0, 0), (2, 1), (0, 1), (1, 0), (1, 1)],
}


def pieces(c, q, b):
    return ([(SEG, c, q, 0)] if b == 0 else []) + [(KV, c, q, b)]


def unit(c, b):
    return pieces(c, 1, b) + pieces(c, 0, b)


def schedule():
    plan = {(c, q): {} for c in range(4) for q in range(2)}

    def put(c, q, step, *acts):
        plan[c, q].setdefault(step, []).extend(acts)

    def send(items, *ways):
        return [("send", i, w) for i in items for w in ways]

    def take(items, *ways):
        return [a for i in items for a in [("wait", i)] + [("send", i, w) for w in ways]]

    for c in range(4):
        put(c, 0, 0, *send(pieces(c, 0, 0) + pieces(c, 0, 1), PART))
        put(c, 0, 1, *take(pieces(c, 1, 0) + pieces(c, 1, 1)))
    own = lambda c: pieces(c, 1, 0) + pieces(c, 1, 1)
    put(0, 1, 0, *send(own(0), NEXT, PREV), *send(own(0), PART))
    put(0, 1, 1, *take(pieces(0, 0, 0) + pieces(0, 0, 1), NEXT, PREV))
    put(0, 1, 1, *take(pieces(1, 1, 1) + pieces(1, 0, 1), PREV))
    put(1, 1, 0, *send(own(1), NEXT), *send(pieces(1, 1, 1), PREV), *send(own(1), PART))
    put(1, 1, 1, *take(pieces(1, 0, 0), NEXT), *take(pieces(1, 0, 1), NEXT, PREV))
    put(1, 1, 2, *take(unit(0, 0), NEXT, PART))
    put(1, 1, 3, *take(unit(0, 1), NEXT, PART))
    put(2, 1, 0, *send(own(2), NEXT), *send(own(2), PART))
    put(2, 1, 1, *take(pieces(2, 0, 0) + pieces(2, 0, 1), NEXT))
    put(2, 1, 2, *take(unit(1, 0), NEXT, PART))
    put(2, 1, 3, *take(unit(1, 1), PART))
    put(2, 1, 4, *take(unit(0, 0), PART))
    put(2, 1, 5, *take(unit(0, 1), PART))
    put(3, 1, 0, *send(own(3), PART))
    put(3, 1, 1, *take(pieces(3, 0, 0)), *take(pieces(3, 0, 1)))
    put(3, 1, 2, *take(unit(2, 0), PART))
    put(3, 1, 3, *take(unit(0, 0), PART))
    put(3, 1, 4, *take(unit(2, 1), PART))
    put(3, 1, 5, *take(unit(0, 1), PART))
    put(3, 1, 6, *take(unit(1, 0), PART))
    put(3, 1, 7, *take(unit(1, 1), PART))
    return plan


PLAN = schedule()


def attend(lhs, kk, vv, state, b, c2, first=False):
    m_ref, l_ref, acc_ref = state
    s = lax.dot_general(lhs, kk, (((1,), (1,)), ((), ())), preferred_element_type=F32)
    m_new = jnp.broadcast_to(jnp.max(jnp.maximum(s[:, :128], s[:, 128:]), axis=1, keepdims=True), (s.shape[0], 128))
    if not first:
        m_prev = m_ref[b]
        m_new = jnp.maximum(m_prev, m_new)
        alpha = jnp.exp2((m_prev - m_new) * c2)
    p0 = jnp.exp2((s[:, :128] - m_new) * c2)
    p1 = jnp.exp2((s[:, 128:] - m_new) * c2)
    m_ref[b] = m_new
    p = jnp.concatenate([p0.astype(BF16), p1.astype(BF16)], axis=1)
    pv = lax.dot_general(p, vv, (((1,), (0,)), ((), ())), preferred_element_type=F32)
    l_ref[b] = p0 + p1 if first else l_ref[b] * alpha + (p0 + p1)
    acc_ref[b] = pv if first else acc_ref[b] * alpha + pv


def branch(index, leaves):
    keys = sorted(leaves)
    if len(keys) == 1:
        pl.when(index == keys[0])(leaves[keys[0]])
        return
    mid = keys[len(keys) // 2]
    pl.when(index < mid)(lambda: branch(index, {k: leaves[k] for k in keys if k < mid}))
    pl.when(index >= mid)(lambda: branch(index, {k: leaves[k] for k in keys if k >= mid}))


def gather_attend(q_hbm, k_hbm, v_hbm, seg_hbm, m_ref, l_ref, acc_ref, qb, oh, kv, bias, sg, qsem, ldsem, ssem, rsem, sssem, srsem):
    me = lax.axis_index("cp")
    chip, core = me // 2, me % 2
    rows = qb.shape[1]
    heads = rows // 128
    c2 = 128**-0.5 * LOG2E

    def slot(item):
        kind, c, q, b = item
        return sg.at[c * 2 + q] if kind == SEG else kv.at[c, q, b]

    loads = [pltpu.make_async_copy(seg_hbm, sg.at[me], ldsem.at[2])]
    for i, src in enumerate((k_hbm, v_hbm)):
        loads.append(pltpu.make_async_copy(src, kv.at[chip, core, :, i], ldsem.at[i]))
    for copy in loads:
        copy.start()
    q_loads = [pltpu.make_async_copy(q_hbm.at[b], qb.at[b], qsem.at[b]) for b in range(2)]
    for copy in q_loads:
        copy.start()

    barrier = pltpu.get_barrier_semaphore()
    next_dev = lax.rem(chip + 1, 4) * 2 + 1
    prev_dev = lax.rem(chip + 3, 4) * 2 + 1
    part_dev = chip * 2 + 1 - core
    pl.semaphore_signal(barrier, inc=1, device_id={"cp": part_dev}, device_id_type=MESH)

    @pl.when(core == 1)
    def _():
        for dev in (next_dev, prev_dev):
            pl.semaphore_signal(barrier, inc=1, device_id={"cp": dev}, device_id_type=MESH)
        pl.semaphore_wait(barrier, 3)

    @pl.when(core == 0)
    def _():
        pl.semaphore_wait(barrier, 1)

    ways = (next_dev, prev_dev, part_dev)

    def remote(item, way):
        kind, c, q, b = item
        sems = (sssem.at[way], srsem.at[c * 2 + q]) if kind == SEG else (ssem, rsem.at[c, q, b])
        ref = slot(item)
        return pltpu.make_async_remote_copy(src_ref=ref, dst_ref=ref, send_sem=sems[0], recv_sem=sems[1], device_id={"cp": ways[way]}, device_id_type=MESH)

    def run(actions):
        for act in actions:
            if act[0] == "wait":
                remote(act[1], PART).wait_recv()
            else:
                remote(act[1], act[2]).start()

    for copy in loads:
        copy.wait()
    branch(me, {c * 2 + q: lambda a=steps[0]: run(a) for (c, q), steps in PLAN.items()})

    def fill(t, _):
        here = lax.broadcasted_iota(jnp.int32, (heads, 128), 1) == t
        oh[pl.ds(pl.multiple_of(t * heads, heads), heads), :] = jnp.where(here, 1.0, 0.0).astype(BF16)
        return 0

    lax.fori_loop(0, 128, fill, 0, unroll=16)
    for copy in q_loads:
        copy.wait()

    def hide(c, b, buf, local=False):
        seg_t = sg[me, pl.ds(b, 1), :].astype(F32)
        for half in range(2):
            seg_u = sg[c * 2 + half, pl.ds(b, 1), :].astype(F32)
            seen = jnp.broadcast_to(seg_u, (128, 128)).T == seg_t
            if local:
                u_pos = half * 128 + lax.broadcasted_iota(jnp.int32, (128, 128), 0)
                t_pos = core * 128 + lax.broadcasted_iota(jnp.int32, (128, 128), 1)
                seen = seen & (u_pos <= t_pos)
            buf[pl.ds(half * 128, 128), :] = jnp.where(seen, 0.0, HIDE).astype(BF16)

    state = (m_ref, l_ref, acc_ref)

    def lhs(b):
        return jnp.concatenate([qb[b], oh[...]], axis=1)

    def keys(c, b, mask):
        kk = jnp.concatenate([kv[c, 0, b, 0], kv[c, 1, b, 0]], axis=0)
        return jnp.concatenate([kk, mask], axis=1), jnp.concatenate([kv[c, 0, b, 1], kv[c, 1, b, 1]], axis=0)

    branch(me, {c * 2 + q: lambda a=steps[1]: run(a) for (c, q), steps in PLAN.items()})
    for b in range(2):
        hide(chip, b, bias.at[b], local=True)
    for b in range(2):
        attend(lhs(b), *keys(chip, b, bias[b]), state, b, c2, first=True)

    def pack(units):
        return sum((c * 2 + b) * 8**i for i, (c, b) in enumerate(units))

    todo = jnp.where(chip == 1, pack(ORDER[1]), jnp.where(chip == 2, pack(ORDER[2]), pack(ORDER[3])))

    def step(s, todo):
        code = todo % 8
        c, b = code // 2, code % 2

        @pl.when(core == 1)
        def _():
            branch(chip, {cc: lambda acts={i: a for i, a in PLAN[cc, 1].items() if i > 1}: branch(s, {i: lambda a=a: run(a) for i, a in acts.items()}) for cc in (1, 2, 3)})

        @pl.when(core == 0)
        def _():
            @pl.when(b == 0)
            def _():
                for q in range(2):
                    remote((SEG, c, q, 0), PART).wait_recv()

            for q in (1, 0):
                remote((KV, c, q, b), PART).wait_recv()

        hide(c, b, bias.at[0])
        attend(lhs(b), *keys(c, b, bias[0]), state, b, c2)
        return todo // 8

    lax.fori_loop(2, 2 * (chip + 1), step, todo)

    def drain(steps):
        sent = [act[1:] for acts in steps.values() for act in acts if act[0] == "send"]
        big = sum(item[0] == KV for item, _ in sent) * 128
        pltpu.make_async_copy(acc_ref.at[0, pl.ds(0, big)], acc_ref.at[0, pl.ds(0, big)], ssem).wait()
        for way in (NEXT, PREV, PART):
            n = sum(item[0] == SEG and w == way for item, w in sent)
            if n:
                pltpu.make_async_copy(sg.at[pl.ds(0, n)], sg.at[pl.ds(0, n)], sssem.at[way]).wait()

    branch(me, {c * 2 + q: lambda steps=steps: drain(steps) for (c, q), steps in PLAN.items()})


def normalise(m_ref, l_ref, acc_ref, o_hbm, lse_hbm, ob, lseb, sem):
    batch, rows, _ = acc_ref.shape
    heads = rows // 128
    chunk = rows // CHUNKS
    lane = lax.broadcasted_iota(jnp.int32, (heads, 128), 1)
    copies = []
    for b in range(batch):
        top = tot = jnp.zeros((heads, 128), F32)
        for i in range(CHUNKS):
            part = pl.ds(i * chunk, chunk)
            total = jnp.broadcast_to(jnp.sum(l_ref[b, part, :], axis=1, keepdims=True), (chunk, 128))
            ob[b, part, :] = (acc_ref[b, part, :] * (1.0 / total)).astype(BF16)
            copies.append(pltpu.make_async_copy(ob.at[b, part], o_hbm.at[b, part], sem.at[b, i]))
            copies[-1].start()
            for j in range(chunk // heads):
                here = lane == i * chunk // heads + j
                top = jnp.where(here, m_ref[b, pl.ds(i * chunk + j * heads, heads), :], top)
                tot = jnp.where(here, total[j * heads : (j + 1) * heads], tot)
        lseb[b] = top * 128**-0.5 + jnp.log(tot)
        copies.append(pltpu.make_async_copy(lseb.at[b], lse_hbm.at[b], sem.at[b, CHUNKS]))
        copies[-1].start()
    for copy in copies:
        copy.wait()


def solution(mesh):
    def local(q, k, v, seg):
        batch, seq, heads, head = q.shape
        rows = seq * heads
        running = pl.pallas_call(
            gather_attend,
            out_shape=(pltpu.VMEM((batch, rows, 128), F32),) * 3,
            in_specs=[pl.BlockSpec(memory_space=pltpu.HBM)] * 4,
            out_specs=(pl.BlockSpec(memory_space=pltpu.VMEM),) * 3,
            scratch_shapes=[
                pltpu.VMEM((batch, rows, head), BF16),
                pltpu.VMEM((rows, 128), BF16),
                pltpu.VMEM((4, 2, batch, 2, seq, head), BF16),
                pltpu.VMEM((2, 2 * seq, 128), BF16),
                pltpu.VMEM((8, batch, seq), jnp.int32),
                pltpu.SemaphoreType.DMA((2,)),
                pltpu.SemaphoreType.DMA((3,)),
                pltpu.SemaphoreType.DMA,
                pltpu.SemaphoreType.DMA((4, 2, 2)),
                pltpu.SemaphoreType.DMA((3,)),
                pltpu.SemaphoreType.DMA((8,)),
            ],
            compiler_params=pltpu.CompilerParams(collective_id=0, has_side_effects=True, vmem_limit_bytes=40 * 2**20),
        )(*[pltpu.with_memory_space_constraint(x, pltpu.HBM) for x in (q.reshape(batch, rows, head), k, v, seg)])
        out, lse = pl.pallas_call(
            normalise,
            out_shape=(jax.ShapeDtypeStruct((batch, rows, head), BF16), jax.ShapeDtypeStruct((batch, heads, seq), F32)),
            in_specs=[pl.BlockSpec(memory_space=pltpu.VMEM)] * 3,
            out_specs=(pl.BlockSpec(memory_space=pltpu.HBM),) * 2,
            scratch_shapes=[
                pltpu.VMEM((batch, rows, head), BF16),
                pltpu.VMEM((batch, heads, seq), F32),
                pltpu.SemaphoreType.DMA((batch, CHUNKS + 1)),
            ],
            compiler_params=pltpu.CompilerParams(vmem_limit_bytes=16 * 2**20),
        )(*running)
        return out.reshape(q.shape), lse.transpose(0, 2, 1)

    return jax.shard_map(
        local,
        mesh=mesh,
        in_specs=(P("dp", "cp", None, None), P("dp", "cp", None), P("dp", "cp", None), P("dp", "cp")),
        out_specs=(P("dp", "cp", None, None), P("dp", "cp", None)),
        check_vma=False,
    )
```

```python
import functools

import jax
import jax.numpy as jnp
import numpy as np
from jax import lax
from jax.experimental import pallas as pl
from jax.experimental.pallas import tpu as pltpu
from jax.sharding import PartitionSpec as P

MESH = pl.DeviceIdType.MESH
F32, BF16 = jnp.float32, jnp.bfloat16
HIDE = float(jnp.finfo(jnp.bfloat16).min)
LOG2E = float(np.log2(np.e))
NEXT, PREV, PART = 0, 1, 2
CHUNKS = 4
KV, SEG = 0, 1

LOADED, READY, OWN0, OWN1, NEAR0, NEAR1, FAR0, FAR1 = range(8)


def pieces(c, q, b):
    return ([(SEG, c, q, 0)] if b == 0 else []) + [(KV, c, q, b)]


def unit(c, b):
    return pieces(c, 1, b) + pieces(c, 0, b)


def schedule():
    plan = {(c, q): {} for c in range(4) for q in range(2)}

    def put(c, q, point, *acts):
        plan[c, q].setdefault(point, []).extend(acts)

    def send(items, *ways):
        return [("send", i, w) for i in items for w in ways]

    def take(items, *ways):
        return [a for i in items for a in [("wait", i)] + [("send", i, w) for w in ways]]

    for c in range(4):
        for q in range(2):
            for b in range(2):
                ways = ([NEXT] if c < 3 else []) + ([PREV] if c == 1 and b == 1 else []) + [PART]
                put(c, q, LOADED, *send(pieces(c, q, b), *ways))
                if c == 0:
                    put(c, q, READY, *send(pieces(c, q, b), PREV))
                put(c, q, OWN0 + b, *take(pieces(c, 1 - q, b)))
            if q == 0:
                near = [unit(c - 1, b) for b in range(2)] if c % 2 else []
                far = [unit(1, b) + unit(0, b) for b in range(2)] if c > 1 else []
                for b, items in enumerate(near):
                    put(c, q, NEAR0 + b, *take(items))
                for b, items in enumerate(far):
                    put(c, q, FAR0 + b, *take(items))
    put(0, 1, OWN0, *take(unit(1, 1), PREV))
    put(1, 1, OWN1, *take(unit(0, 0), NEXT, PART))
    put(1, 1, NEAR0, *take(unit(0, 1), NEXT, PART))
    put(2, 1, FAR0, *take(unit(1, 0), NEXT, PART), *take(unit(1, 1) + unit(0, 0), PART))
    put(2, 1, FAR1, *take(unit(0, 1), PART))
    put(3, 1, NEAR0, *take(unit(2, 0), PART))
    put(3, 1, NEAR1, *take(unit(2, 1) + unit(0, 0), PART))
    put(3, 1, FAR0, *take(unit(1, 0) + unit(0, 1), PART))
    put(3, 1, FAR1, *take(unit(1, 1), PART))
    return plan


PLAN = schedule()


def attend(lhs, kk, vv, state, b, c2, first=False):
    m_ref, l_ref, acc_ref = state
    s = lax.dot_general(lhs, kk, (((1,), (1,)), ((), ())), preferred_element_type=F32)
    parts = [s[:, i : i + 128] for i in range(0, s.shape[1], 128)]
    m_new = jnp.broadcast_to(jnp.max(functools.reduce(jnp.maximum, parts), axis=1, keepdims=True), (s.shape[0], 128))
    if not first:
        m_prev = m_ref[b]
        m_new = jnp.maximum(m_prev, m_new)
        alpha = jnp.exp2((m_prev - m_new) * c2)
    parts = [jnp.exp2((x - m_new) * c2) for x in parts]
    m_ref[b] = m_new
    total = functools.reduce(jnp.add, parts)
    l_ref[b] = total if first else l_ref[b] * alpha + total
    p = jnp.concatenate([x.astype(BF16) for x in parts], axis=1)
    pv = lax.dot_general(p, vv, (((1,), (0,)), ((), ())), preferred_element_type=F32)
    acc_ref[b] = pv if first else acc_ref[b] * alpha + pv


def branch(index, leaves):
    keys = sorted(leaves)
    if len(keys) == 1:
        pl.when(index == keys[0])(leaves[keys[0]])
        return
    mid = keys[len(keys) // 2]
    pl.when(index < mid)(lambda: branch(index, {k: leaves[k] for k in keys if k < mid}))
    pl.when(index >= mid)(lambda: branch(index, {k: leaves[k] for k in keys if k >= mid}))


def gather_attend(q_hbm, k_hbm, v_hbm, seg_hbm, m_ref, l_ref, acc_ref, qb, oh, kv, bias, sg, qsem, ldsem, ssem, rsem, sssem, srsem, ready):
    me = lax.axis_index("cp")
    chip, core = me // 2, me % 2
    rows = qb.shape[1]
    heads = rows // 128
    c2 = 128**-0.5 * LOG2E

    def slot(item):
        kind, c, q, b = item
        return sg.at[c * 2 + q] if kind == SEG else kv.at[c, q, b]

    loads = [pltpu.make_async_copy(seg_hbm, sg.at[me], ldsem.at[2])]
    for i, src in enumerate((k_hbm, v_hbm)):
        loads.append(pltpu.make_async_copy(src, kv.at[chip, core, :, i], ldsem.at[i]))
    for copy in loads:
        copy.start()
    q_loads = [pltpu.make_async_copy(q_hbm.at[b], qb.at[b], qsem.at[b]) for b in range(2)]
    for copy in q_loads:
        copy.start()

    barrier = pltpu.get_barrier_semaphore()
    next_dev = lax.rem(chip + 1, 4) * 2 + 1
    prev_dev = lax.rem(chip + 3, 4) * 2 + 1
    part_dev = chip * 2 + 1 - core

    def greet(*devs):
        for dev in devs:
            pl.semaphore_signal(barrier, inc=1, device_id={"cp": dev}, device_id_type=MESH)

    greet(part_dev)
    pl.when((core == 1) & (chip > 0))(lambda: greet(prev_dev, prev_dev - 1))
    pl.when((core == 1) & (chip == 0))(lambda: greet(next_dev, next_dev - 1))
    pl.when(chip == 0)(lambda: greet(prev_dev))
    for i, n in {0: 2, 1: 2, 2: 3, 3: 3, 4: 2, 5: 2, 6: 1, 7: 3}.items():
        pl.when(me == i)(lambda n=n: pl.semaphore_wait(barrier, n))

    @pl.when(me == 7)
    def _():
        for dev in (next_dev, next_dev - 1):
            pl.semaphore_signal(ready, inc=1, device_id={"cp": dev}, device_id_type=MESH)

    ways = (next_dev, prev_dev, part_dev)

    def remote(item, way):
        kind, c, q, b = item
        sems = (sssem.at[way], srsem.at[c * 2 + q]) if kind == SEG else (ssem, rsem.at[c, q, b])
        ref = slot(item)
        return pltpu.make_async_remote_copy(src_ref=ref, dst_ref=ref, send_sem=sems[0], recv_sem=sems[1], device_id={"cp": ways[way]}, device_id_type=MESH)

    def run(actions):
        for act in actions:
            if act[0] == "wait":
                remote(act[1], PART).wait_recv()
            else:
                remote(act[1], act[2]).start()

    for copy in loads:
        copy.wait()
    def at(point):
        acts = {c * 2 + q: points[point] for (c, q), points in PLAN.items() if point in points}
        branch(me, {i: lambda a=a: run(a) for i, a in acts.items()})

    at(LOADED)

    @pl.when(chip == 0)
    def _():
        pl.semaphore_wait(ready, 1)
        at(READY)

    def fill(t, _):
        here = lax.broadcasted_iota(jnp.int32, (heads, 128), 1) == t
        oh[pl.ds(pl.multiple_of(t * heads, heads), heads), :] = jnp.where(here, 1.0, 0.0).astype(BF16)
        return 0

    lax.fori_loop(0, 128, fill, 0, unroll=16)
    for copy in q_loads:
        copy.wait()

    def hide(c, b, buf, local=False):
        seg_t = sg[me, pl.ds(b, 1), :].astype(F32)
        for half in range(2):
            seg_u = sg[c * 2 + half, pl.ds(b, 1), :].astype(F32)
            seen = jnp.broadcast_to(seg_u, (128, 128)).T == seg_t
            if local:
                u_pos = half * 128 + lax.broadcasted_iota(jnp.int32, (128, 128), 0)
                t_pos = core * 128 + lax.broadcasted_iota(jnp.int32, (128, 128), 1)
                seen = seen & (u_pos <= t_pos)
            buf[pl.ds(half * 128, 128), :] = jnp.where(seen, 0.0, HIDE).astype(BF16)

    state = (m_ref, l_ref, acc_ref)

    def lhs(b):
        return jnp.concatenate([qb[b], oh[...]], axis=1)

    def keys(c, b, mask):
        kk = jnp.concatenate([kv[c, 0, b, 0], kv[c, 1, b, 0]], axis=0)
        return jnp.concatenate([kk, mask], axis=1), jnp.concatenate([kv[c, 0, b, 1], kv[c, 1, b, 1]], axis=0)

    for b in range(2):
        at(OWN0 + b)
        hide(chip, b, bias.at[0], local=True)
        attend(lhs(b), *keys(chip, b, bias[0]), state, b, c2, first=True)

    @pl.when(chip % 2 == 1)
    def _():
        def near(b, _):
            pl.when(b == 0)(lambda: at(NEAR0))
            pl.when(b == 1)(lambda: at(NEAR1))
            hide(chip - 1, b, bias.at[0])
            attend(lhs(b), *keys(chip - 1, b, bias[0]), state, b, c2)
            return 0

        lax.fori_loop(0, 2, near, 0)

    @pl.when(chip > 1)
    def _():
        def far(b, _):
            pl.when(b == 0)(lambda: at(FAR0))
            pl.when(b == 1)(lambda: at(FAR1))
            parts = []
            for c in range(2):
                hide(c, b, bias.at[c])
                parts.append(keys(c, b, bias[c]))
            attend(lhs(b), *[jnp.concatenate(x, axis=0) for x in zip(*parts, strict=True)], state, b, c2)
            return 0

        lax.fori_loop(0, 2, far, 0)

    def drain(steps):
        sent = [act[1:] for acts in steps.values() for act in acts if act[0] == "send"]
        big = sum(item[0] == KV for item, _ in sent) * 128
        pltpu.make_async_copy(acc_ref.at[0, pl.ds(0, big)], acc_ref.at[0, pl.ds(0, big)], ssem).wait()
        for way in (NEXT, PREV, PART):
            n = sum(item[0] == SEG and w == way for item, w in sent)
            if n:
                pltpu.make_async_copy(sg.at[pl.ds(0, n)], sg.at[pl.ds(0, n)], sssem.at[way]).wait()

    branch(me, {c * 2 + q: lambda steps=steps: drain(steps) for (c, q), steps in PLAN.items()})


def normalise(m_ref, l_ref, acc_ref, o_hbm, lse_hbm, ob, lseb, sem):
    batch, rows, _ = acc_ref.shape
    heads = rows // 128
    chunk = rows // CHUNKS
    lane = lax.broadcasted_iota(jnp.int32, (heads, 128), 1)
    copies = []
    for b in range(batch):
        top = tot = jnp.zeros((heads, 128), F32)
        for i in range(CHUNKS):
            part = pl.ds(i * chunk, chunk)
            total = jnp.broadcast_to(jnp.sum(l_ref[b, part, :], axis=1, keepdims=True), (chunk, 128))
            ob[b, part, :] = (acc_ref[b, part, :] * (1.0 / total)).astype(BF16)
            copies.append(pltpu.make_async_copy(ob.at[b, part], o_hbm.at[b, part], sem.at[b, i]))
            copies[-1].start()
            for j in range(chunk // heads):
                here = lane == i * chunk // heads + j
                top = jnp.where(here, m_ref[b, pl.ds(i * chunk + j * heads, heads), :], top)
                tot = jnp.where(here, total[j * heads : (j + 1) * heads], tot)
        lseb[b] = top * 128**-0.5 + jnp.log(tot)
        copies.append(pltpu.make_async_copy(lseb.at[b], lse_hbm.at[b], sem.at[b, CHUNKS]))
        copies[-1].start()
    for copy in copies:
        copy.wait()


def solution(mesh):
    def local(q, k, v, seg):
        batch, seq, heads, head = q.shape
        rows = seq * heads
        running = pl.pallas_call(
            gather_attend,
            out_shape=(pltpu.VMEM((batch, rows, 128), F32),) * 3,
            in_specs=[pl.BlockSpec(memory_space=pltpu.HBM)] * 4,
            out_specs=(pl.BlockSpec(memory_space=pltpu.VMEM),) * 3,
            scratch_shapes=[
                pltpu.VMEM((batch, rows, head), BF16),
                pltpu.VMEM((rows, 128), BF16),
                pltpu.VMEM((4, 2, batch, 2, seq, head), BF16),
                pltpu.VMEM((2, 2 * seq, 128), BF16),
                pltpu.VMEM((8, batch, seq), jnp.int32),
                pltpu.SemaphoreType.DMA((2,)),
                pltpu.SemaphoreType.DMA((3,)),
                pltpu.SemaphoreType.DMA,
                pltpu.SemaphoreType.DMA((4, 2, 2)),
                pltpu.SemaphoreType.DMA((3,)),
                pltpu.SemaphoreType.DMA((8,)),
                pltpu.SemaphoreType.REGULAR,
            ],
            compiler_params=pltpu.CompilerParams(collective_id=0, has_side_effects=True, vmem_limit_bytes=40 * 2**20),
        )(*[pltpu.with_memory_space_constraint(x, pltpu.HBM) for x in (q.reshape(batch, rows, head), k, v, seg)])
        out, lse = pl.pallas_call(
            normalise,
            out_shape=(jax.ShapeDtypeStruct((batch, rows, head), BF16), jax.ShapeDtypeStruct((batch, heads, seq), F32)),
            in_specs=[pl.BlockSpec(memory_space=pltpu.VMEM)] * 3,
            out_specs=(pl.BlockSpec(memory_space=pltpu.HBM),) * 2,
            scratch_shapes=[
                pltpu.VMEM((batch, rows, head), BF16),
                pltpu.VMEM((batch, heads, seq), F32),
                pltpu.SemaphoreType.DMA((batch, CHUNKS + 1)),
            ],
            compiler_params=pltpu.CompilerParams(vmem_limit_bytes=16 * 2**20),
        )(*running)
        return out.reshape(q.shape), lse.transpose(0, 2, 1)

    return jax.shard_map(
        local,
        mesh=mesh,
        in_specs=(P("dp", "cp", None, None), P("dp", "cp", None), P("dp", "cp", None), P("dp", "cp")),
        out_specs=(P("dp", "cp", None, None), P("dp", "cp", None)),
        check_vma=False,
    )
```

```python
import functools

import jax
import jax.numpy as jnp
import numpy as np
from jax import lax
from jax.experimental import pallas as pl
from jax.experimental.pallas import tpu as pltpu
from jax.sharding import PartitionSpec as P

MESH = pl.DeviceIdType.MESH
F32, BF16 = jnp.float32, jnp.bfloat16
HIDE = float(jnp.finfo(jnp.bfloat16).min)
LOG2E = float(np.log2(np.e))
NEXT, PREV, PART = 0, 1, 2
CHUNKS = 4
KV, SEG = 0, 1

IDS, LOADED, READY, OWN_IDS, OWN0, OWN1, NEAR_IDS, NEAR0, FAR_IDS, NEAR1, FAR0, FAR1 = range(12)


def unit(c, b):
    return [(KV, c, 1, b), (KV, c, 0, b)]


def ids(c):
    return [(SEG, c, 1, 0), (SEG, c, 0, 0)]


def schedule():
    plan = {(c, q): {} for c in range(4) for q in range(2)}

    def put(c, q, point, *acts):
        plan[c, q].setdefault(point, []).extend(acts)

    def send(items, *ways):
        return [("send", i, w) for i in items for w in ways]

    def take(items, *ways):
        return [a for i in items for a in [("wait", i)] + [("send", i, w) for w in ways]]

    for c in range(4):
        for q in range(2):
            on = [NEXT] if c < 3 else []
            put(c, q, IDS, *send([(SEG, c, q, 0)], *on, PART))
            put(c, q, OWN_IDS, *take([(SEG, c, 1 - q, 0)]))
            for b in range(2):
                put(c, q, LOADED, *send([(KV, c, q, b)], *on, *([PREV] if (c, q, b) == (1, 0, 1) else []), PART))
                put(c, q, OWN0 + b, *take([(KV, c, 1 - q, b)]))
            if c == 0:
                put(c, q, READY, *send([(SEG, c, q, 0), (KV, c, q, 0), (KV, c, q, 1)], PREV))
            if q == 0:
                if c % 2:
                    put(c, q, NEAR_IDS, *take(ids(c - 1)))
                    put(c, q, NEAR0, *take(unit(c - 1, 0)))
                    put(c, q, NEAR1, *take(unit(c - 1, 1)))
                if c > 1:
                    put(c, q, FAR_IDS, *take(ids(0) + ids(1)))
                    for b in range(2):
                        put(c, q, FAR0 + b, *take(unit(0, b) + unit(1, b)))
    put(0, 1, OWN0, *take([(KV, 1, 0, 1)], PREV))
    put(1, 1, OWN1, *take(ids(0) + unit(0, 0), NEXT, PART))
    put(1, 1, NEAR0, *take(unit(0, 1), NEXT, PART))
    put(2, 1, OWN1, *take(ids(1), NEXT, PART))
    put(2, 1, FAR_IDS, *take(unit(1, 0) + [(KV, 1, 1, 1)], NEXT, PART), *take(ids(0), PART))
    put(2, 1, FAR0, *take([(KV, 1, 0, 1)] + unit(0, 0), PART))
    put(2, 1, FAR1, *take(unit(0, 1), PART))
    put(3, 1, OWN1, *take(ids(2), PART))
    put(3, 1, NEAR0, *take(unit(2, 0), PART))
    put(3, 1, FAR_IDS, *take(unit(2, 1) + ids(0) + ids(1), PART))
    put(3, 1, FAR0, *take(unit(0, 0) + unit(1, 0) + unit(0, 1) + unit(1, 1), PART))
    return plan


PLAN = schedule()


def attend(lhs, kk, vv, state, b, c2, first=False):
    m_ref, l_ref, acc_ref = state
    s = lax.dot_general(lhs, kk, (((1,), (1,)), ((), ())), preferred_element_type=F32)
    parts = [s[:, i : i + 128] for i in range(0, s.shape[1], 128)]
    m_new = jnp.broadcast_to(jnp.max(functools.reduce(jnp.maximum, parts), axis=1, keepdims=True), (s.shape[0], 128))
    if not first:
        m_prev = m_ref[b]
        m_new = jnp.maximum(m_prev, m_new)
        alpha = jnp.exp2((m_prev - m_new) * c2)
    parts = [jnp.exp2((x - m_new) * c2) for x in parts]
    m_ref[b] = m_new
    total = functools.reduce(jnp.add, parts)
    l_ref[b] = total if first else l_ref[b] * alpha + total
    p = jnp.concatenate([x.astype(BF16) for x in parts], axis=1)
    pv = lax.dot_general(p, vv, (((1,), (0,)), ((), ())), preferred_element_type=F32)
    acc_ref[b] = pv if first else acc_ref[b] * alpha + pv


def branch(index, leaves):
    keys = sorted(leaves)
    if len(keys) == 1:
        pl.when(index == keys[0])(leaves[keys[0]])
        return
    mid = keys[len(keys) // 2]
    pl.when(index < mid)(lambda: branch(index, {k: leaves[k] for k in keys if k < mid}))
    pl.when(index >= mid)(lambda: branch(index, {k: leaves[k] for k in keys if k >= mid}))


def gather_attend(q_hbm, k_hbm, v_hbm, seg_hbm, m_ref, l_ref, acc_ref, qb, oh, kv, bias, far_bias, sg, qsem, ldsem, ssem, rsem, sssem, srsem, ready):
    me = lax.axis_index("cp")
    chip, core = me // 2, me % 2
    rows = qb.shape[1]
    heads = rows // 128
    c2 = 128**-0.5 * LOG2E

    def slot(item):
        kind, c, q, b = item
        return sg.at[c * 2 + q] if kind == SEG else kv.at[c, q, b]

    loads = [pltpu.make_async_copy(seg_hbm, sg.at[me], ldsem.at[2])]
    for i, src in enumerate((k_hbm, v_hbm)):
        loads.append(pltpu.make_async_copy(src, kv.at[chip, core, :, i], ldsem.at[i]))
    for copy in loads:
        copy.start()
    q_loads = [pltpu.make_async_copy(q_hbm.at[b], qb.at[b], qsem.at[b]) for b in range(2)]
    for copy in q_loads:
        copy.start()

    barrier = pltpu.get_barrier_semaphore()
    next_dev = lax.rem(chip + 1, 4) * 2 + 1
    prev_dev = lax.rem(chip + 3, 4) * 2 + 1
    part_dev = chip * 2 + 1 - core

    def greet(*devs):
        for dev in devs:
            pl.semaphore_signal(barrier, inc=1, device_id={"cp": dev}, device_id_type=MESH)

    greet(part_dev)
    pl.when((core == 1) & (chip > 0))(lambda: greet(prev_dev, prev_dev - 1))
    pl.when((core == 1) & (chip == 0))(lambda: greet(next_dev, next_dev - 1))
    pl.when(chip == 0)(lambda: greet(prev_dev))
    for i, n in {0: 2, 1: 2, 2: 3, 3: 3, 4: 2, 5: 2, 6: 1, 7: 3}.items():
        pl.when(me == i)(lambda n=n: pl.semaphore_wait(barrier, n))

    @pl.when(me == 7)
    def _():
        for dev in (next_dev, next_dev - 1):
            pl.semaphore_signal(ready, inc=1, device_id={"cp": dev}, device_id_type=MESH)

    ways = (next_dev, prev_dev, part_dev)

    def remote(item, way):
        kind, c, q, b = item
        sems = (sssem.at[way], srsem.at[c * 2 + q]) if kind == SEG else (ssem, rsem.at[c, q, b])
        ref = slot(item)
        return pltpu.make_async_remote_copy(src_ref=ref, dst_ref=ref, send_sem=sems[0], recv_sem=sems[1], device_id={"cp": ways[way]}, device_id_type=MESH)

    def run(actions):
        for act in actions:
            if act[0] == "wait":
                remote(act[1], PART).wait_recv()
            else:
                remote(act[1], act[2]).start()

    def at(point):
        acts = {c * 2 + q: points[point] for (c, q), points in PLAN.items() if point in points}
        branch(me, {i: lambda a=a: run(a) for i, a in acts.items()})

    loads[0].wait()
    at(IDS)
    for copy in loads[1:]:
        copy.wait()
    at(LOADED)

    @pl.when(chip == 0)
    def _():
        pl.semaphore_wait(ready, 1)
        at(READY)

    def fill(t, _):
        here = lax.broadcasted_iota(jnp.int32, (heads, 128), 1) == t
        oh[pl.ds(pl.multiple_of(t * heads, heads), heads), :] = jnp.where(here, 1.0, 0.0).astype(BF16)
        return 0

    lax.fori_loop(0, 128, fill, 0, unroll=16)
    for copy in q_loads:
        copy.wait()

    def hide(c, b, buf, local=False):
        seg_t = sg[me, pl.ds(b, 1), :].astype(F32)
        for half in range(2):
            seg_u = sg[c * 2 + half, pl.ds(b, 1), :].astype(F32)
            seen = jnp.broadcast_to(seg_u, (128, 128)).T == seg_t
            if local:
                u_pos = half * 128 + lax.broadcasted_iota(jnp.int32, (128, 128), 0)
                t_pos = core * 128 + lax.broadcasted_iota(jnp.int32, (128, 128), 1)
                seen = seen & (u_pos <= t_pos)
            buf[pl.ds(half * 128, 128), :] = jnp.where(seen, 0.0, HIDE).astype(BF16)

    state = (m_ref, l_ref, acc_ref)

    def lhs(b):
        return jnp.concatenate([qb[b], oh[...]], axis=1)

    def keys(c, b, mask):
        kk = jnp.concatenate([kv[c, 0, b, 0], kv[c, 1, b, 0]], axis=0)
        return jnp.concatenate([kk, mask], axis=1), jnp.concatenate([kv[c, 0, b, 1], kv[c, 1, b, 1]], axis=0)

    def hide_far():
        for b in range(2):
            for c in range(2):
                hide(c, b, far_bias.at[b, c])

    at(OWN_IDS)
    for b in range(2):
        hide(chip, b, bias.at[b], local=True)
    for b in range(2):
        at(OWN0 + b)
        attend(lhs(b), *keys(chip, b, bias[b]), state, b, c2, first=True)

    @pl.when(chip % 2 == 1)
    def _():
        at(NEAR_IDS)
        for b in range(2):
            hide(chip - 1, b, bias.at[b])
        at(NEAR0)
        attend(lhs(0), *keys(chip - 1, 0, bias[0]), state, 0, c2)

    @pl.when(chip > 1)
    def _():
        at(FAR_IDS)
        hide_far()

    @pl.when(chip % 2 == 1)
    def _():
        at(NEAR1)
        attend(lhs(1), *keys(chip - 1, 1, bias[1]), state, 1, c2)

    @pl.when(chip > 1)
    def _():
        for b in range(2):
            at(FAR0 + b)
            parts = [keys(c, b, far_bias[b, c]) for c in range(2)]
            attend(lhs(b), *[jnp.concatenate(x, axis=0) for x in zip(*parts, strict=True)], state, b, c2)

    def drain(steps):
        sent = [act[1:] for acts in steps.values() for act in acts if act[0] == "send"]
        big = sum(item[0] == KV for item, _ in sent) * 128
        pltpu.make_async_copy(acc_ref.at[0, pl.ds(0, big)], acc_ref.at[0, pl.ds(0, big)], ssem).wait()
        for way in (NEXT, PREV, PART):
            n = sum(item[0] == SEG and w == way for item, w in sent)
            if n:
                pltpu.make_async_copy(sg.at[pl.ds(0, n)], sg.at[pl.ds(0, n)], sssem.at[way]).wait()

    branch(me, {c * 2 + q: lambda steps=steps: drain(steps) for (c, q), steps in PLAN.items()})


def normalise(m_ref, l_ref, acc_ref, o_hbm, lse_hbm, ob, lseb, sem):
    batch, rows, _ = acc_ref.shape
    heads = rows // 128
    chunk = rows // CHUNKS
    lane = lax.broadcasted_iota(jnp.int32, (heads, 128), 1)
    copies = []
    for b in range(batch):
        top = tot = jnp.zeros((heads, 128), F32)
        for i in range(CHUNKS):
            part = pl.ds(i * chunk, chunk)
            total = jnp.broadcast_to(jnp.sum(l_ref[b, part, :], axis=1, keepdims=True), (chunk, 128))
            ob[b, part, :] = (acc_ref[b, part, :] * (1.0 / total)).astype(BF16)
            copies.append(pltpu.make_async_copy(ob.at[b, part], o_hbm.at[b, part], sem.at[b, i]))
            copies[-1].start()
            for j in range(chunk // heads):
                here = lane == i * chunk // heads + j
                top = jnp.where(here, m_ref[b, pl.ds(i * chunk + j * heads, heads), :], top)
                tot = jnp.where(here, total[j * heads : (j + 1) * heads], tot)
        lseb[b] = top * 128**-0.5 + jnp.log(tot)
        copies.append(pltpu.make_async_copy(lseb.at[b], lse_hbm.at[b], sem.at[b, CHUNKS]))
        copies[-1].start()
    for copy in copies:
        copy.wait()


def solution(mesh):
    def local(q, k, v, seg):
        batch, seq, heads, head = q.shape
        rows = seq * heads
        running = pl.pallas_call(
            gather_attend,
            out_shape=(pltpu.VMEM((batch, rows, 128), F32),) * 3,
            in_specs=[pl.BlockSpec(memory_space=pltpu.HBM)] * 4,
            out_specs=(pl.BlockSpec(memory_space=pltpu.VMEM),) * 3,
            scratch_shapes=[
                pltpu.VMEM((batch, rows, head), BF16),
                pltpu.VMEM((rows, 128), BF16),
                pltpu.VMEM((4, 2, batch, 2, seq, head), BF16),
                pltpu.VMEM((2, 2 * seq, 128), BF16),
                pltpu.VMEM((2, 2, 2 * seq, 128), BF16),
                pltpu.VMEM((8, batch, seq), jnp.int32),
                pltpu.SemaphoreType.DMA((2,)),
                pltpu.SemaphoreType.DMA((3,)),
                pltpu.SemaphoreType.DMA,
                pltpu.SemaphoreType.DMA((4, 2, 2)),
                pltpu.SemaphoreType.DMA((3,)),
                pltpu.SemaphoreType.DMA((8,)),
                pltpu.SemaphoreType.REGULAR,
            ],
            compiler_params=pltpu.CompilerParams(collective_id=0, has_side_effects=True, vmem_limit_bytes=40 * 2**20),
        )(*[pltpu.with_memory_space_constraint(x, pltpu.HBM) for x in (q.reshape(batch, rows, head), k, v, seg)])
        out, lse = pl.pallas_call(
            normalise,
            out_shape=(jax.ShapeDtypeStruct((batch, rows, head), BF16), jax.ShapeDtypeStruct((batch, heads, seq), F32)),
            in_specs=[pl.BlockSpec(memory_space=pltpu.VMEM)] * 3,
            out_specs=(pl.BlockSpec(memory_space=pltpu.HBM),) * 2,
            scratch_shapes=[
                pltpu.VMEM((batch, rows, head), BF16),
                pltpu.VMEM((batch, heads, seq), F32),
                pltpu.SemaphoreType.DMA((batch, CHUNKS + 1)),
            ],
            compiler_params=pltpu.CompilerParams(vmem_limit_bytes=16 * 2**20),
        )(*running)
        return out.reshape(q.shape), lse.transpose(0, 2, 1)

    return jax.shard_map(
        local,
        mesh=mesh,
        in_specs=(P("dp", "cp", None, None), P("dp", "cp", None), P("dp", "cp", None), P("dp", "cp")),
        out_specs=(P("dp", "cp", None, None), P("dp", "cp", None)),
        check_vma=False,
    )
```

```python
import functools

import jax
import jax.numpy as jnp
import numpy as np
from jax import lax
from jax.experimental import pallas as pl
from jax.experimental.pallas import tpu as pltpu
from jax.sharding import PartitionSpec as P

MESH = pl.DeviceIdType.MESH
F32, BF16 = jnp.float32, jnp.bfloat16
HIDE = float(jnp.finfo(jnp.bfloat16).min)
LOG2E = float(np.log2(np.e))
NEXT, PREV, PART = 0, 1, 2
CHUNKS = 4
KV, SEG = 0, 1

IDS, LOADED, READY, OWN_IDS, OWN0, OWN1, NEAR_IDS, NEAR0, NEAR1, FAR_IDS, FAR0, FAR1, FAR2 = range(13)


def unit(c, b):
    return (KV, c, (1, 0), b)


def ids(c):
    return (SEG, c, (1, 0), 0)


def schedule():
    plan = {(c, q): {} for c in range(4) for q in range(2)}

    def put(c, q, point, *acts):
        plan[c, q].setdefault(point, []).extend(acts)

    def send(piece, *ways):
        return [("send", piece, w) for w in ways]

    def take(group, *ways):
        kind, c, qs, b = group
        return [("wait", group)] + [a for q in qs for a in send((kind, c, q, b), *ways)]

    for c in range(4):
        for q in range(2):
            on = [NEXT] if c < 3 else []
            put(c, q, IDS, *send((SEG, c, q, 0), *on, PART))
            put(c, q, OWN_IDS, *take((SEG, c, (1 - q,), 0)))
            for b in range(2):
                put(c, q, LOADED, *send((KV, c, q, b), *on, *([PREV] if (c, q, b) == (1, 0, 1) else []), PART))
                put(c, q, OWN0 + b, *take((KV, c, (1 - q,), b)))
            if c == 0:
                put(c, q, READY, *send((SEG, c, q, 0), PREV), *send((KV, c, q, 0), PREV), *send((KV, c, q, 1), PREV))
            if q == 0:
                if c:
                    put(c, q, NEAR_IDS, *take(ids(c - 1)))
                    put(c, q, NEAR0, *take(unit(c - 1, 0)))
                    put(c, q, NEAR1, *take(unit(c - 1, 1)))
                if c > 1:
                    put(c, q, FAR_IDS, *take(ids(0)))
                    put(c, q, FAR0, *take(unit(0, 0)))
                if c == 2:
                    put(c, q, FAR1, *take(unit(0, 1)))
                if c == 3:
                    put(c, q, FAR_IDS, *take(ids(1)))
                    put(c, q, FAR1, *take(unit(1, 0)))
                    put(c, q, FAR2, *take(unit(0, 1)), *take(unit(1, 1)))
    put(0, 1, OWN0, *take((KV, 1, (0,), 1), PREV))
    put(1, 1, OWN1, *take(ids(0), NEXT, PART), *take(unit(0, 0), NEXT, PART))
    put(1, 1, NEAR0, *take(unit(0, 1), NEXT, PART))
    put(2, 1, OWN1, *take(ids(1), NEXT, PART))
    put(2, 1, NEAR0, *take(unit(1, 0), NEXT, PART))
    put(2, 1, NEAR1, *take(unit(1, 1), PART), *send((KV, 1, 1, 1), NEXT), *take(ids(0), PART))
    put(2, 1, FAR0, *take(unit(0, 0), PART))
    put(2, 1, FAR1, *take(unit(0, 1), PART))
    put(3, 1, OWN1, *take(ids(2), PART))
    put(3, 1, NEAR0, *take(unit(2, 0), PART))
    put(3, 1, NEAR1, *take(unit(2, 1), PART), *take(ids(0), PART), *take(ids(1), PART))
    put(3, 1, FAR_IDS, *take(unit(0, 0), PART))
    put(3, 1, FAR1, *take(unit(1, 0), PART), *take(unit(0, 1), PART), *take(unit(1, 1), PART))
    return plan


PLAN = schedule()


def attend(lhs, kk, vv, state, b, c2, first=False):
    m_ref, l_ref, acc_ref = state
    s = lax.dot_general(lhs, kk, (((1,), (1,)), ((), ())), preferred_element_type=F32)
    parts = [s[:, i : i + 128] for i in range(0, s.shape[1], 128)]
    m_new = jnp.broadcast_to(jnp.max(functools.reduce(jnp.maximum, parts), axis=1, keepdims=True), (s.shape[0], 128))
    if not first:
        m_prev = m_ref[b]
        m_new = jnp.maximum(m_prev, m_new)
        alpha = jnp.exp2((m_prev - m_new) * c2)
    parts = [jnp.exp2((x - m_new) * c2) for x in parts]
    m_ref[b] = m_new
    total = functools.reduce(jnp.add, parts)
    l_ref[b] = total if first else l_ref[b] * alpha + total
    p = jnp.concatenate([x.astype(BF16) for x in parts], axis=1)
    pv = lax.dot_general(p, vv, (((1,), (0,)), ((), ())), preferred_element_type=F32)
    acc_ref[b] = pv if first else acc_ref[b] * alpha + pv


def branch(index, leaves):
    keys = sorted(leaves)
    if len(keys) == 1:
        pl.when(index == keys[0])(leaves[keys[0]])
        return
    mid = keys[len(keys) // 2]
    pl.when(index < mid)(lambda: branch(index, {k: leaves[k] for k in keys if k < mid}))
    pl.when(index >= mid)(lambda: branch(index, {k: leaves[k] for k in keys if k >= mid}))


def gather_attend(q_hbm, k_hbm, v_hbm, seg_hbm, m_ref, l_ref, acc_ref, first_sum, qb, oh, kv, bias, far_bias, sg, ldsem, ssem, rsem, srsem, ready):
    me = lax.axis_index("cp")
    chip, core = me // 2, me % 2
    rows = qb.shape[1]
    heads = rows // 128
    c2 = 128**-0.5 * LOG2E

    def slot(item):
        kind, c, q, b = item
        return sg.at[c * 2 + q] if kind == SEG else kv.at[c, q, b]

    pltpu.make_async_copy(seg_hbm, sg.at[me], ldsem.at[0]).start()
    for i, src in enumerate((k_hbm, v_hbm)):
        pltpu.make_async_copy(src, kv.at[chip, core, :, i], ldsem.at[1]).start()
    q_load = pltpu.make_async_copy(q_hbm, qb, ldsem.at[2])
    q_load.start()

    def wait(ref, sem):
        pltpu.make_async_copy(ref, ref, sem).wait()

    barrier = pltpu.get_barrier_semaphore()
    next_dev = lax.rem(chip + 1, 4) * 2 + 1
    prev_dev = lax.rem(chip + 3, 4) * 2 + 1
    part_dev = chip * 2 + 1 - core

    def greet(*devs):
        for dev in devs:
            pl.semaphore_signal(barrier, inc=1, device_id={"cp": dev}, device_id_type=MESH)

    greet(part_dev)
    pl.when((core == 1) & (chip > 0))(lambda: greet(prev_dev, prev_dev - 1))
    pl.when((core == 1) & (chip == 0))(lambda: greet(next_dev, next_dev - 1))
    pl.when(chip == 0)(lambda: greet(prev_dev))
    for i, n in {0: 2, 1: 2, 2: 3, 3: 3, 4: 2, 5: 2, 6: 1, 7: 3}.items():
        pl.when(me == i)(lambda n=n: pl.semaphore_wait(barrier, n))

    @pl.when(me == 7)
    def _():
        for dev in (next_dev, next_dev - 1):
            pl.semaphore_signal(ready, inc=1, device_id={"cp": dev}, device_id_type=MESH)

    ways = (next_dev, prev_dev, part_dev)

    def run(actions):
        for act in actions:
            kind, c, q, b = act[1]
            arrival = srsem.at[c] if kind == SEG else rsem.at[c, b]
            if act[0] == "send":
                ref, left = slot(act[1]), ssem.at[kind]
                pltpu.make_async_remote_copy(src_ref=ref, dst_ref=ref, send_sem=left, recv_sem=arrival, device_id={"cp": ways[act[2]]}, device_id_type=MESH).start()
            elif kind == SEG:
                wait(sg.at[pl.ds(0, len(q))], arrival)
            else:
                wait(kv.at[c, pl.ds(0, len(q)), b], arrival)

    def at(point):
        acts = {c * 2 + q: points[point] for (c, q), points in PLAN.items() if point in points}
        branch(me, {i: lambda a=a: run(a) for i, a in acts.items()})

    wait(sg.at[me], ldsem.at[0])
    at(IDS)
    wait(kv.at[chip, core], ldsem.at[1])
    at(LOADED)

    @pl.when(chip == 0)
    def _():
        pl.semaphore_wait(ready, 1)
        at(READY)

    def fill(t, _):
        here = lax.broadcasted_iota(jnp.int32, (heads, 128), 1) == t
        oh[pl.ds(pl.multiple_of(t * heads, heads), heads), :] = jnp.where(here, 1.0, 0.0).astype(BF16)
        return 0

    lax.fori_loop(0, 128, fill, 0, unroll=16)
    q_load.wait()

    key = lax.broadcasted_iota(jnp.int32, (128, 128), 0)

    def hide(c, b, buf, local=False):
        seg_t = sg[me, pl.ds(b, 1), :]
        for half in range(2):
            seg_u = sg[c * 2 + half, pl.ds(b, 1), :]
            below = [jnp.broadcast_to(jnp.sum(jnp.where(seg_u < i, 1.0, 0.0), axis=1, keepdims=True), (1, 128)) for i in (1, 2)]
            smaller = jnp.where(seg_t == 0, 0.0, jnp.where(seg_t == 1, below[0], below[1])).astype(jnp.int32)
            seen = key >= smaller
            if local:
                t_pos = core * 128 + lax.broadcasted_iota(jnp.int32, (1, 128), 1)
                seen = seen & (key <= t_pos - half * 128)
            buf[pl.ds(half * 128, 128), :] = jnp.where(seen, 0.0, HIDE).astype(BF16)

    state = (m_ref, l_ref, acc_ref)

    def lhs(b):
        return jnp.concatenate([qb[b], oh[...]], axis=1)

    def keys(c, b, mask):
        kk = jnp.concatenate([kv[c, 0, b, 0], kv[c, 1, b, 0]], axis=0)
        return jnp.concatenate([kk, mask], axis=1), jnp.concatenate([kv[c, 0, b, 1], kv[c, 1, b, 1]], axis=0)

    def hide_far():
        for b in range(2):
            for c in range(2):
                hide(c, b, far_bias.at[b, c])

    at(OWN_IDS)
    for b in range(2):
        hide(chip, b, bias.at[b], local=True)
    for b in range(2):
        at(OWN0 + b)
        attend(lhs(b), *keys(chip, b, bias[b]), state, b, c2, first=True)

    def sum_first():
        first_sum[...] = jnp.broadcast_to(jnp.sum(l_ref[0], axis=1, keepdims=True), (rows, 128))

    def one(c, b, mask):
        attend(lhs(b), *keys(c, b, mask), state, b, c2)

    @pl.when(chip > 0)
    def _():
        at(NEAR_IDS)
        for b in range(2):
            hide(chip - 1, b, bias.at[b])
        for b in range(2):
            at(NEAR0 + b)
            one(chip - 1, b, bias[b])

    @pl.when(chip > 1)
    def _():
        at(FAR_IDS)
        hide_far()
        at(FAR0)
        one(0, 0, far_bias[0, 0])
        at(FAR1)
        unit1 = chip - 2
        one(unit1, 1 - unit1, far_bias[1 - unit1, unit1])

    @pl.when(chip > 2)
    def _():
        at(FAR2)
        sum_first()
        parts = [keys(c, 1, far_bias[1, c]) for c in range(2)]
        attend(lhs(1), *[jnp.concatenate(x, axis=0) for x in zip(*parts, strict=True)], state, 1, c2)

    pl.when(chip < 3)(sum_first)

    def drain(steps):
        sent = [act[1][0] for acts in steps.values() for act in acts if act[0] == "send"]
        wait(acc_ref.at[0, pl.ds(0, sent.count(KV) * 128)], ssem.at[KV])
        wait(sg.at[pl.ds(0, sent.count(SEG))], ssem.at[SEG])

    branch(me, {c * 2 + q: lambda steps=steps: drain(steps) for (c, q), steps in PLAN.items()})


def normalise(m_ref, l_ref, acc_ref, first_sum, o_hbm, lse_hbm, ob, lseb, sem):
    batch, rows, _ = acc_ref.shape
    heads = rows // 128
    chunk = rows // CHUNKS
    lane = lax.broadcasted_iota(jnp.int32, (heads, 128), 1)
    copies = []
    for b in range(batch):
        top = tot = jnp.zeros((heads, 128), F32)
        for i in range(CHUNKS):
            part = pl.ds(i * chunk, chunk)
            if b == 0:
                total = first_sum[part, :]
            else:
                total = jnp.broadcast_to(jnp.sum(l_ref[b, part, :], axis=1, keepdims=True), (chunk, 128))
            ob[b, part, :] = (acc_ref[b, part, :] * (1.0 / total)).astype(BF16)
            copies.append(pltpu.make_async_copy(ob.at[b, part], o_hbm.at[b, part], sem.at[b, i]))
            copies[-1].start()
            for j in range(chunk // heads):
                here = lane == i * chunk // heads + j
                top = jnp.where(here, m_ref[b, pl.ds(i * chunk + j * heads, heads), :], top)
                tot = jnp.where(here, total[j * heads : (j + 1) * heads], tot)
        lseb[b] = top * 128**-0.5 + jnp.log(tot)
        copies.append(pltpu.make_async_copy(lseb.at[b], lse_hbm.at[b], sem.at[b, CHUNKS]))
        copies[-1].start()
    for copy in copies:
        copy.wait()


def solution(mesh):
    def local(q, k, v, seg):
        batch, seq, heads, head = q.shape
        rows = seq * heads
        running = pl.pallas_call(
            gather_attend,
            out_shape=(pltpu.VMEM((batch, rows, 128), F32),) * 3 + (pltpu.VMEM((rows, 128), F32),),
            in_specs=[pl.BlockSpec(memory_space=pltpu.HBM)] * 4,
            out_specs=(pl.BlockSpec(memory_space=pltpu.VMEM),) * 4,
            scratch_shapes=[
                pltpu.VMEM((batch, rows, head), BF16),
                pltpu.VMEM((rows, 128), BF16),
                pltpu.VMEM((4, 2, batch, 2, seq, head), BF16),
                pltpu.VMEM((2, 2 * seq, 128), BF16),
                pltpu.VMEM((2, 2, 2 * seq, 128), BF16),
                pltpu.VMEM((8, batch, seq), jnp.int32),
                pltpu.SemaphoreType.DMA((3,)),
                pltpu.SemaphoreType.DMA((2,)),
                pltpu.SemaphoreType.DMA((4, 2)),
                pltpu.SemaphoreType.DMA((4,)),
                pltpu.SemaphoreType.REGULAR,
            ],
            compiler_params=pltpu.CompilerParams(collective_id=0, has_side_effects=True, vmem_limit_bytes=40 * 2**20),
        )(*[pltpu.with_memory_space_constraint(x, pltpu.HBM) for x in (q.reshape(batch, rows, head), k, v, seg)])
        out, lse = pl.pallas_call(
            normalise,
            out_shape=(jax.ShapeDtypeStruct((batch, rows, head), BF16), jax.ShapeDtypeStruct((batch, heads, seq), F32)),
            in_specs=[pl.BlockSpec(memory_space=pltpu.VMEM)] * 4,
            out_specs=(pl.BlockSpec(memory_space=pltpu.HBM),) * 2,
            scratch_shapes=[
                pltpu.VMEM((batch, rows, head), BF16),
                pltpu.VMEM((batch, heads, seq), F32),
                pltpu.SemaphoreType.DMA((batch, CHUNKS + 1)),
            ],
            compiler_params=pltpu.CompilerParams(vmem_limit_bytes=16 * 2**20),
        )(*running)
        return out.reshape(q.shape), lse.transpose(0, 2, 1)

    return jax.shard_map(
        local,
        mesh=mesh,
        in_specs=(P("dp", "cp", None, None), P("dp", "cp", None), P("dp", "cp", None), P("dp", "cp")),
        out_specs=(P("dp", "cp", None, None), P("dp", "cp", None)),
        check_vma=False,
    )
```

```python
import functools

import jax
import jax.numpy as jnp
import numpy as np
from jax import lax
from jax.experimental import pallas as pl
from jax.experimental.pallas import tpu as pltpu
from jax.sharding import PartitionSpec as P

MESH = pl.DeviceIdType.MESH
F32, BF16 = jnp.float32, jnp.bfloat16
HIDE = float(jnp.finfo(jnp.bfloat16).min)
LOG2E = float(np.log2(np.e))
NEXT, PREV, PART = 0, 1, 2
CHUNKS = 4
KV, SEG = 0, 1

IDS, LOADED, READY, OWN_IDS, OWN0, OWN1, NEAR_IDS, NEAR0, NEAR1, FAR0, FAR1, FAR2 = range(12)


def unit(c, b):
    return (KV, c, (1, 0), b)


def ids(c):
    return (SEG, c, (1, 0), 0)


def schedule():
    plan = {(c, q): {} for c in range(4) for q in range(2)}

    def put(c, q, point, *acts):
        plan[c, q].setdefault(point, []).extend(acts)

    def send(piece, *ways):
        return [("send", piece, w) for w in ways]

    def take(group, *ways):
        kind, c, qs, b = group
        return [("wait", group)] + [a for q in qs for a in send((kind, c, q, b), *ways)]

    for c in range(4):
        for q in range(2):
            on = [NEXT] if c < 3 else []
            put(c, q, IDS, *send((SEG, c, q, 0), *on, PART))
            put(c, q, OWN_IDS, *take((SEG, c, (1 - q,), 0)))
            for b in range(2):
                put(c, q, LOADED, *send((KV, c, q, b), *on, *([PREV] if (c, q, b) == (1, 0, 1) else []), PART))
                put(c, q, OWN0 + b, *take((KV, c, (1 - q,), b)))
            if c == 0:
                put(c, q, READY, *send((SEG, c, q, 0), PREV), *send((KV, c, q, 0), PREV), *send((KV, c, q, 1), PREV))
            if q == 0:
                if c:
                    put(c, q, NEAR_IDS, *take(ids(c - 1)))
                    put(c, q, NEAR0, *take(unit(c - 1, 0)))
                    put(c, q, NEAR1, *take(unit(c - 1, 1)))
                if c > 1:
                    put(c, q, NEAR1, *take(ids(0)))
                    put(c, q, FAR0, *take(unit(0, 0)))
                if c == 2:
                    put(c, q, FAR1, *take(unit(0, 1)))
                if c == 3:
                    put(c, q, NEAR1, *take(ids(1)))
                    put(c, q, FAR1, *take(unit(1, 0)))
                    put(c, q, FAR2, *take(unit(0, 1)), *take(unit(1, 1)))
    put(0, 1, OWN0, *take((KV, 1, (0,), 1), PREV))
    put(1, 1, OWN1, *take(ids(0), NEXT, PART), *take(unit(0, 0), NEXT, PART))
    put(1, 1, NEAR0, *take(unit(0, 1), NEXT, PART))
    put(2, 1, OWN1, *take(ids(1), NEXT, PART))
    put(2, 1, NEAR0, *take(unit(1, 0), NEXT, PART))
    put(2, 1, NEAR1, *take(unit(1, 1), PART), *send((KV, 1, 1, 1), NEXT), *take(ids(0), PART))
    put(2, 1, FAR0, *take(unit(0, 0), PART))
    put(2, 1, FAR1, *take(unit(0, 1), PART))
    put(3, 1, OWN1, *take(ids(2), PART))
    put(3, 1, NEAR0, *take(unit(2, 0), PART))
    put(3, 1, NEAR1, *take(unit(2, 1), PART), *take(ids(0), PART), *take(ids(1), PART))
    put(3, 1, FAR0, *take(unit(0, 0), PART))
    put(3, 1, FAR1, *take(unit(1, 0), PART), *take(unit(0, 1), PART), *take(unit(1, 1), PART))
    return plan


PLAN = schedule()


def attend(lhs, kk, vv, state, b, c2, first=False):
    m_ref, l_ref, acc_ref = state
    s = lax.dot_general(lhs, kk, (((1,), (1,)), ((), ())), preferred_element_type=F32)
    parts = [s[:, i : i + 128] for i in range(0, s.shape[1], 128)]
    m_new = jnp.broadcast_to(jnp.max(functools.reduce(jnp.maximum, parts), axis=1, keepdims=True), (s.shape[0], 128))
    if not first:
        m_prev = m_ref[b]
        m_new = jnp.maximum(m_prev, m_new)
        alpha = jnp.exp2((m_prev - m_new) * c2)
    parts = [jnp.exp2((x - m_new) * c2) for x in parts]
    m_ref[b] = m_new
    total = functools.reduce(jnp.add, parts)
    l_ref[b] = total if first else l_ref[b] * alpha + total
    p = jnp.concatenate([x.astype(BF16) for x in parts], axis=1)
    pv = lax.dot_general(p, vv, (((1,), (0,)), ((), ())), preferred_element_type=F32)
    acc_ref[b] = pv if first else acc_ref[b] * alpha + pv


def branch(index, leaves):
    keys = sorted(leaves)
    if len(keys) == 1:
        pl.when(index == keys[0])(leaves[keys[0]])
        return
    mid = keys[len(keys) // 2]
    pl.when(index < mid)(lambda: branch(index, {k: leaves[k] for k in keys if k < mid}))
    pl.when(index >= mid)(lambda: branch(index, {k: leaves[k] for k in keys if k >= mid}))


def gather_attend(q_hbm, k_hbm, v_hbm, seg_hbm, m_ref, l_ref, acc_ref, first_sum, qb, oh, kv, bias, far_bias, sg, ldsem, ssem, rsem, srsem, ready):
    me = lax.axis_index("cp")
    chip, core = me // 2, me % 2
    rows = qb.shape[1]
    heads = rows // 128
    c2 = 128**-0.5 * LOG2E

    def slot(item):
        kind, c, q, b = item
        return sg.at[c * 2 + q] if kind == SEG else kv.at[c, q, b]

    def wait(ref, sem):
        pltpu.make_async_copy(ref, ref, sem).wait()

    barrier = pltpu.get_barrier_semaphore()
    next_dev = lax.rem(chip + 1, 4) * 2 + 1
    prev_dev = lax.rem(chip + 3, 4) * 2 + 1
    part_dev = chip * 2 + 1 - core

    def greet(*devs):
        for dev in devs:
            pl.semaphore_signal(barrier, inc=1, device_id={"cp": dev}, device_id_type=MESH)

    greet(part_dev)
    pl.when((core == 1) & (chip > 0))(lambda: greet(prev_dev, prev_dev - 1))
    pl.when((core == 1) & (chip == 0))(lambda: greet(next_dev, next_dev - 1))
    pl.when(chip == 0)(lambda: greet(prev_dev))
    pltpu.make_async_copy(seg_hbm, sg.at[me], ldsem.at[0]).start()
    for i, src in enumerate((k_hbm, v_hbm)):
        pltpu.make_async_copy(src, kv.at[chip, core, :, i], ldsem.at[1]).start()
    q_load = pltpu.make_async_copy(q_hbm, qb, ldsem.at[2])
    q_load.start()

    for i, n in {0: 2, 1: 2, 2: 3, 3: 3, 4: 2, 5: 2, 6: 1, 7: 3}.items():
        pl.when(me == i)(lambda n=n: pl.semaphore_wait(barrier, n))

    @pl.when(me == 7)
    def _():
        for dev in (next_dev, next_dev - 1):
            pl.semaphore_signal(ready, inc=1, device_id={"cp": dev}, device_id_type=MESH)

    ways = (next_dev, prev_dev, part_dev)

    def run(actions):
        for act in actions:
            kind, c, q, b = act[1]
            arrival = srsem.at[c] if kind == SEG else rsem.at[c, b]
            if act[0] == "send":
                ref, left = slot(act[1]), ssem.at[kind]
                pltpu.make_async_remote_copy(src_ref=ref, dst_ref=ref, send_sem=left, recv_sem=arrival, device_id={"cp": ways[act[2]]}, device_id_type=MESH).start()
            elif kind == SEG:
                wait(sg.at[pl.ds(0, len(q))], arrival)
            else:
                wait(kv.at[c, pl.ds(0, len(q)), b], arrival)

    def at(point):
        acts = {c * 2 + q: points[point] for (c, q), points in PLAN.items() if point in points}
        branch(me, {i: lambda a=a: run(a) for i, a in acts.items()})

    wait(sg.at[me], ldsem.at[0])
    at(IDS)
    wait(kv.at[chip, core], ldsem.at[1])
    at(LOADED)

    @pl.when(chip == 0)
    def _():
        pl.semaphore_wait(ready, 1)
        at(READY)

    def fill(t, _):
        here = lax.broadcasted_iota(jnp.int32, (heads, 128), 1) == t
        oh[pl.ds(pl.multiple_of(t * heads, heads), heads), :] = jnp.where(here, 1.0, 0.0).astype(BF16)
        return 0

    lax.fori_loop(0, 128, fill, 0, unroll=16)
    q_load.wait()

    key = lax.broadcasted_iota(jnp.int32, (128, 128), 0)

    def hide(c, b, buf, local=False):
        seg_t = sg[me, pl.ds(b, 1), :]
        for half in range(2):
            seg_u = sg[c * 2 + half, pl.ds(b, 1), :]
            below = [jnp.broadcast_to(jnp.sum(jnp.where(seg_u < i, 1.0, 0.0), axis=1, keepdims=True), (1, 128)) for i in (1, 2)]
            smaller = jnp.where(seg_t == 0, 0.0, jnp.where(seg_t == 1, below[0], below[1])).astype(jnp.int32)
            seen = key >= smaller
            if local:
                t_pos = core * 128 + lax.broadcasted_iota(jnp.int32, (1, 128), 1)
                seen = seen & (key <= t_pos - half * 128)
            buf[pl.ds(half * 128, 128), :] = jnp.where(seen, 0.0, HIDE).astype(BF16)

    state = (m_ref, l_ref, acc_ref)

    def lhs(b):
        return jnp.concatenate([qb[b], oh[...]], axis=1)

    def keys(c, b, mask):
        kk = jnp.concatenate([kv[c, 0, b, 0], kv[c, 1, b, 0]], axis=0)
        return jnp.concatenate([kk, mask], axis=1), jnp.concatenate([kv[c, 0, b, 1], kv[c, 1, b, 1]], axis=0)

    def hide_far(c, b):
        hide(c, b, far_bias.at[b, c])

    at(OWN_IDS)
    for b in range(2):
        hide(chip, b, bias.at[b], local=True)
    for b in range(2):
        at(OWN0 + b)
        attend(lhs(b), *keys(chip, b, bias[b]), state, b, c2, first=True)

    def sum_first():
        first_sum[...] = jnp.broadcast_to(jnp.sum(l_ref[0], axis=1, keepdims=True), (rows, 128))

    def one(c, b, mask):
        attend(lhs(b), *keys(c, b, mask), state, b, c2)

    @pl.when(chip > 0)
    def _():
        at(NEAR_IDS)
        for b in range(2):
            hide(chip - 1, b, bias.at[b])
        at(NEAR0)
        one(chip - 1, 0, bias[0])
        at(NEAR1)
        hide_far(0, 0)
        one(chip - 1, 1, bias[1])

    @pl.when(chip > 1)
    def _():
        at(FAR0)
        hide_far(1, 0)
        hide_far(0, 1)
        one(0, 0, far_bias[0, 0])
        at(FAR1)
        hide_far(1, 1)
        unit1 = chip - 2
        one(unit1, 1 - unit1, far_bias[1 - unit1, unit1])

    @pl.when(chip > 2)
    def _():
        at(FAR2)
        sum_first()
        parts = [keys(c, 1, far_bias[1, c]) for c in range(2)]
        attend(lhs(1), *[jnp.concatenate(x, axis=0) for x in zip(*parts, strict=True)], state, 1, c2)

    pl.when(chip < 3)(sum_first)

    def drain(steps):
        sent = [act[1][0] for acts in steps.values() for act in acts if act[0] == "send"]
        wait(acc_ref.at[0, pl.ds(0, sent.count(KV) * 128)], ssem.at[KV])
        wait(sg.at[pl.ds(0, sent.count(SEG))], ssem.at[SEG])

    branch(me, {c * 2 + q: lambda steps=steps: drain(steps) for (c, q), steps in PLAN.items()})


def normalise(m_ref, l_ref, acc_ref, first_sum, o_hbm, lse_hbm, ob, lseb, sem):
    batch, rows, _ = acc_ref.shape
    heads = rows // 128
    chunk = rows // CHUNKS
    lane = lax.broadcasted_iota(jnp.int32, (heads, 128), 1)
    copies = []
    for b in range(batch):
        top = tot = jnp.zeros((heads, 128), F32)
        for i in range(CHUNKS):
            part = pl.ds(i * chunk, chunk)
            if b == 0:
                total = first_sum[part, :]
            else:
                total = jnp.broadcast_to(jnp.sum(l_ref[b, part, :], axis=1, keepdims=True), (chunk, 128))
            ob[b, part, :] = (acc_ref[b, part, :] * (1.0 / total)).astype(BF16)
            copies.append(pltpu.make_async_copy(ob.at[b, part], o_hbm.at[b, part], sem.at[b, i]))
            copies[-1].start()
            for j in range(chunk // heads):
                here = lane == i * chunk // heads + j
                top = jnp.where(here, m_ref[b, pl.ds(i * chunk + j * heads, heads), :], top)
                tot = jnp.where(here, total[j * heads : (j + 1) * heads], tot)
        lseb[b] = top * 128**-0.5 + jnp.log(tot)
        copies.append(pltpu.make_async_copy(lseb.at[b], lse_hbm.at[b], sem.at[b, CHUNKS]))
        copies[-1].start()
    for copy in copies:
        copy.wait()


def solution(mesh):
    def local(q, k, v, seg):
        batch, seq, heads, head = q.shape
        rows = seq * heads
        running = pl.pallas_call(
            gather_attend,
            out_shape=(pltpu.VMEM((batch, rows, 128), F32),) * 3 + (pltpu.VMEM((rows, 128), F32),),
            in_specs=[pl.BlockSpec(memory_space=pltpu.HBM)] * 4,
            out_specs=(pl.BlockSpec(memory_space=pltpu.VMEM),) * 4,
            scratch_shapes=[
                pltpu.VMEM((batch, rows, head), BF16),
                pltpu.VMEM((rows, 128), BF16),
                pltpu.VMEM((4, 2, batch, 2, seq, head), BF16),
                pltpu.VMEM((2, 2 * seq, 128), BF16),
                pltpu.VMEM((2, 2, 2 * seq, 128), BF16),
                pltpu.VMEM((8, batch, seq), jnp.int32),
                pltpu.SemaphoreType.DMA((3,)),
                pltpu.SemaphoreType.DMA((2,)),
                pltpu.SemaphoreType.DMA((4, 2)),
                pltpu.SemaphoreType.DMA((4,)),
                pltpu.SemaphoreType.REGULAR,
            ],
            compiler_params=pltpu.CompilerParams(collective_id=0, has_side_effects=True, vmem_limit_bytes=40 * 2**20),
        )(*[pltpu.with_memory_space_constraint(x, pltpu.HBM) for x in (q.reshape(batch, rows, head), k, v, seg)])
        out, lse = pl.pallas_call(
            normalise,
            out_shape=(jax.ShapeDtypeStruct((batch, rows, head), BF16), jax.ShapeDtypeStruct((batch, heads, seq), F32)),
            in_specs=[pl.BlockSpec(memory_space=pltpu.VMEM)] * 4,
            out_specs=(pl.BlockSpec(memory_space=pltpu.HBM),) * 2,
            scratch_shapes=[
                pltpu.VMEM((batch, rows, head), BF16),
                pltpu.VMEM((batch, heads, seq), F32),
                pltpu.SemaphoreType.DMA((batch, CHUNKS + 1)),
            ],
            compiler_params=pltpu.CompilerParams(vmem_limit_bytes=16 * 2**20),
        )(*running)
        return out.reshape(q.shape), lse.transpose(0, 2, 1)

    return jax.shard_map(
        local,
        mesh=mesh,
        in_specs=(P("dp", "cp", None, None), P("dp", "cp", None), P("dp", "cp", None), P("dp", "cp")),
        out_specs=(P("dp", "cp", None, None), P("dp", "cp", None)),
        check_vma=False,
    )
```

```python
import functools

import jax
import jax.numpy as jnp
import numpy as np
from jax import lax
from jax.experimental import pallas as pl
from jax.experimental.pallas import tpu as pltpu
from jax.sharding import PartitionSpec as P

MESH = pl.DeviceIdType.MESH
F32, BF16 = jnp.float32, jnp.bfloat16
HIDE = float(jnp.finfo(jnp.bfloat16).min)
LOG2E = float(np.log2(np.e))
NEXT, PREV, PART = 0, 1, 2
CHUNKS = 4
KV, SEG = 0, 1

IDS, LOADED, READY, OWN_IDS, OWN0, OWN1, NEAR_IDS, NEAR0, NEAR1, FAR0, FAR1, FAR2 = range(12)


def unit(c, b):
    return (KV, c, (1, 0), b)


def ids(c):
    return (SEG, c, (1, 0), 0)


def schedule():
    plan = {(c, q): {} for c in range(4) for q in range(2)}

    def put(c, q, point, *acts):
        plan[c, q].setdefault(point, []).extend(acts)

    def send(piece, *ways):
        return [("send", piece, w) for w in ways]

    def take(group, *ways):
        kind, c, qs, b = group
        return [("wait", group)] + [a for q in qs for a in send((kind, c, q, b), *ways)]

    for c in range(4):
        for q in range(2):
            on = [NEXT] if c < 3 else []
            put(c, q, IDS, *send((SEG, c, q, 0), *on, PART))
            put(c, q, OWN_IDS, *take((SEG, c, (1 - q,), 0)))
            for b in range(2):
                put(c, q, LOADED, *send((KV, c, q, b), *on, *([PREV] if (c, q, b) == (1, 0, 1) else []), PART))
                put(c, q, OWN0 + b, *take((KV, c, (1 - q,), b)))
            if c == 0:
                put(c, q, READY, *send((SEG, c, q, 0), PREV), *send((KV, c, q, 0), PREV), *send((KV, c, q, 1), PREV))
            if q == 0:
                if c:
                    put(c, q, NEAR_IDS, *take(ids(c - 1)))
                    put(c, q, NEAR0, *take(unit(c - 1, 0)))
                    put(c, q, NEAR1, *take(unit(c - 1, 1)))
                if c > 1:
                    put(c, q, NEAR1, *take(ids(0)))
                    put(c, q, FAR0, *take(unit(0, 0)))
                if c == 2:
                    put(c, q, FAR1, *take(unit(0, 1)))
                if c == 3:
                    put(c, q, NEAR1, *take(ids(1)))
                    put(c, q, FAR1, *take(unit(1, 0)))
                    put(c, q, FAR2, *take(unit(0, 1)), *take(unit(1, 1)))
    put(0, 1, OWN0, *take((KV, 1, (0,), 1), PREV))
    put(1, 1, OWN1, *take(ids(0), NEXT, PART), *take(unit(0, 0), NEXT, PART))
    put(1, 1, NEAR0, *take(unit(0, 1), NEXT, PART))
    put(2, 1, OWN1, *take(ids(1), NEXT, PART))
    put(2, 1, NEAR0, *take(unit(1, 0), NEXT, PART))
    put(2, 1, NEAR1, *take(unit(1, 1), PART), *send((KV, 1, 1, 1), NEXT), *take(ids(0), PART))
    put(2, 1, FAR0, *take(unit(0, 0), PART))
    put(2, 1, FAR1, *take(unit(0, 1), PART))
    put(3, 1, OWN1, *take(ids(2), PART))
    put(3, 1, NEAR0, *take(unit(2, 0), PART))
    put(3, 1, NEAR1, *take(unit(2, 1), PART), *take(ids(0), PART), *take(ids(1), PART))
    put(3, 1, FAR0, *take(unit(0, 0), PART))
    put(3, 1, FAR1, *take(unit(1, 0), PART), *take(unit(0, 1), PART), *take(unit(1, 1), PART))
    return plan


PLAN = schedule()


def attend(lhs, kk, vv, state, b, c2, first=False):
    m_ref, l_ref, acc_ref = state
    s = lax.dot_general(lhs, kk, (((1,), (1,)), ((), ())), preferred_element_type=F32)
    parts = [s[:, i : i + 128] for i in range(0, s.shape[1], 128)]
    m_new = jnp.broadcast_to(jnp.max(functools.reduce(jnp.maximum, parts), axis=1, keepdims=True), (s.shape[0], 128))
    if not first:
        m_prev = m_ref[b]
        m_new = jnp.maximum(m_prev, m_new)
        alpha = jnp.exp2((m_prev - m_new) * c2)
    parts = [jnp.exp2((x - m_new) * c2) for x in parts]
    m_ref[b] = m_new
    total = functools.reduce(jnp.add, parts)
    l_ref[b] = total if first else l_ref[b] * alpha + total
    p = jnp.concatenate([x.astype(BF16) for x in parts], axis=1)
    pv = lax.dot_general(p, vv, (((1,), (0,)), ((), ())), preferred_element_type=F32)
    acc_ref[b] = pv if first else acc_ref[b] * alpha + pv


def branch(index, leaves):
    keys = sorted(leaves)
    if len(keys) == 1:
        pl.when(index == keys[0])(leaves[keys[0]])
        return
    mid = keys[len(keys) // 2]
    pl.when(index < mid)(lambda: branch(index, {k: leaves[k] for k in keys if k < mid}))
    pl.when(index >= mid)(lambda: branch(index, {k: leaves[k] for k in keys if k >= mid}))


def gather_attend(q_hbm, k_hbm, v_hbm, seg_hbm, m_ref, l_ref, acc_ref, first_sum, qb, oh, kv, bias, far_bias, sg, ldsem, ssem, rsem, srsem, ready):
    me = lax.axis_index("cp")
    chip, core = me // 2, me % 2
    rows = qb.shape[1]
    heads = rows // 128
    c2 = 128**-0.5 * LOG2E

    def slot(item):
        kind, c, q, b = item
        return sg.at[c * 2 + q] if kind == SEG else kv.at[c, q, b]

    def wait(ref, sem):
        pltpu.make_async_copy(ref, ref, sem).wait()

    barrier = pltpu.get_barrier_semaphore()
    next_dev = lax.rem(chip + 1, 4) * 2 + 1
    prev_dev = lax.rem(chip + 3, 4) * 2 + 1
    part_dev = chip * 2 + 1 - core

    def greet(*devs):
        for dev in devs:
            pl.semaphore_signal(barrier, inc=1, device_id={"cp": dev}, device_id_type=MESH)

    greet(part_dev)
    pl.when((core == 1) & (chip > 0))(lambda: greet(prev_dev, prev_dev - 1))
    pl.when((core == 1) & (chip == 0))(lambda: greet(next_dev, next_dev - 1))
    pl.when(chip == 0)(lambda: greet(prev_dev))
    pltpu.make_async_copy(seg_hbm, sg.at[me], ldsem.at[0]).start()
    for i, src in enumerate((k_hbm, v_hbm)):
        pltpu.make_async_copy(src, kv.at[chip, core, :, i], ldsem.at[1]).start()
    q_load = pltpu.make_async_copy(q_hbm, qb, ldsem.at[2])
    q_load.start()

    for i, n in {0: 2, 1: 2, 2: 3, 3: 3, 4: 2, 5: 2, 6: 1, 7: 3}.items():
        pl.when(me == i)(lambda n=n: pl.semaphore_wait(barrier, n))

    @pl.when(me == 7)
    def _():
        for dev in (next_dev, next_dev - 1):
            pl.semaphore_signal(ready, inc=1, device_id={"cp": dev}, device_id_type=MESH)

    ways = (next_dev, prev_dev, part_dev)

    def run(actions):
        for act in actions:
            kind, c, q, b = act[1]
            arrival = srsem.at[c] if kind == SEG else rsem.at[c, b]
            if act[0] == "send":
                ref, left = slot(act[1]), ssem.at[kind]
                pltpu.make_async_remote_copy(src_ref=ref, dst_ref=ref, send_sem=left, recv_sem=arrival, device_id={"cp": ways[act[2]]}, device_id_type=MESH).start()
            elif kind == SEG:
                wait(sg.at[pl.ds(0, len(q))], arrival)
            else:
                wait(kv.at[c, pl.ds(0, len(q)), b], arrival)

    def at(point):
        acts = {c * 2 + q: points[point] for (c, q), points in PLAN.items() if point in points}
        branch(me, {i: lambda a=a: run(a) for i, a in acts.items()})

    wait(sg.at[me], ldsem.at[0])
    at(IDS)
    wait(kv.at[chip, core], ldsem.at[1])
    at(LOADED)

    @pl.when(chip == 0)
    def _():
        pl.semaphore_wait(ready, 1)
        at(READY)

    def fill(t, _):
        here = lax.broadcasted_iota(jnp.int32, (heads, 128), 1) == t
        oh[pl.ds(pl.multiple_of(t * heads, heads), heads), :] = jnp.where(here, 1.0, 0.0).astype(BF16)
        return 0

    lax.fori_loop(0, 128, fill, 0, unroll=16)
    q_load.wait()

    key = lax.broadcasted_iota(jnp.int32, (128, 128), 0)

    def hide(c, b, buf, local=False):
        seg_t = sg[me, pl.ds(b, 1), :]
        for half in range(2):
            seg_u = sg[c * 2 + half, pl.ds(b, 1), :]
            below = [jnp.broadcast_to(jnp.sum(jnp.where(seg_u < i, 1.0, 0.0), axis=1, keepdims=True), (1, 128)) for i in (1, 2)]
            smaller = jnp.where(seg_t == 0, 0.0, jnp.where(seg_t == 1, below[0], below[1])).astype(jnp.int32)
            seen = key >= smaller
            if local:
                t_pos = core * 128 + lax.broadcasted_iota(jnp.int32, (1, 128), 1)
                seen = seen & (key <= t_pos - half * 128)
            buf[pl.ds(half * 128, 128), :] = jnp.where(seen, 0.0, HIDE).astype(BF16)

    state = (m_ref, l_ref, acc_ref)

    def lhs(b):
        return jnp.concatenate([qb[b], oh[...]], axis=1)

    def keys(c, b, mask):
        kk = jnp.concatenate([kv[c, 0, b, 0], kv[c, 1, b, 0]], axis=0)
        return jnp.concatenate([kk, mask], axis=1), jnp.concatenate([kv[c, 0, b, 1], kv[c, 1, b, 1]], axis=0)

    def hide_far(c, b):
        hide(c, b, far_bias.at[b, c])

    at(OWN_IDS)
    for b in range(2):
        hide(chip, b, bias.at[b], local=True)
    for b in range(2):
        at(OWN0 + b)
        attend(lhs(b), *keys(chip, b, bias[b]), state, b, c2, first=True)

    def drain(steps):
        sent = [act[1][0] for acts in steps.values() for act in acts if act[0] == "send"]
        wait(acc_ref.at[0, pl.ds(0, sent.count(KV) * 128)], ssem.at[KV])
        wait(sg.at[pl.ds(0, sent.count(SEG))], ssem.at[SEG])

    def drained(core):
        branch(chip, {c: lambda steps=PLAN[c, core]: drain(steps) for c in range(4)})

    pl.when(core == 0)(lambda: drained(0))

    def sum_first():
        first_sum[...] = jnp.broadcast_to(jnp.sum(l_ref[0], axis=1, keepdims=True), (rows, 128))

    def one(c, b, mask):
        attend(lhs(b), *keys(c, b, mask), state, b, c2)

    @pl.when(chip > 0)
    def _():
        at(NEAR_IDS)
        for b in range(2):
            hide(chip - 1, b, bias.at[b])
        at(NEAR0)
        one(chip - 1, 0, bias[0])
        at(NEAR1)
        hide_far(0, 0)
        one(chip - 1, 1, bias[1])

    @pl.when(chip > 1)
    def _():
        at(FAR0)
        hide_far(1, 0)
        hide_far(0, 1)
        one(0, 0, far_bias[0, 0])
        at(FAR1)
        hide_far(1, 1)
        unit1 = chip - 2
        one(unit1, 1 - unit1, far_bias[1 - unit1, unit1])

    @pl.when(chip > 2)
    def _():
        at(FAR2)
        sum_first()
        parts = [keys(c, 1, far_bias[1, c]) for c in range(2)]
        attend(lhs(1), *[jnp.concatenate(x, axis=0) for x in zip(*parts, strict=True)], state, 1, c2)

    pl.when(chip < 3)(sum_first)

    pl.when(core == 1)(lambda: drained(1))


def normalise(m_ref, l_ref, acc_ref, first_sum, o_hbm, lse_hbm, ob, lseb, sem):
    batch, rows, _ = acc_ref.shape
    heads = rows // 128
    chunk = rows // CHUNKS
    lane = lax.broadcasted_iota(jnp.int32, (heads, 128), 1)
    copies = []
    for b in range(batch):
        top = tot = jnp.zeros((heads, 128), F32)
        for i in range(CHUNKS):
            part = pl.ds(i * chunk, chunk)
            if b == 0:
                total = first_sum[part, :]
            else:
                total = jnp.broadcast_to(jnp.sum(l_ref[b, part, :], axis=1, keepdims=True), (chunk, 128))
            ob[b, part, :] = (acc_ref[b, part, :] * (1.0 / total)).astype(BF16)
            copies.append(pltpu.make_async_copy(ob.at[b, part], o_hbm.at[b, part], sem.at[b, i]))
            copies[-1].start()
            for j in range(chunk // heads):
                here = lane == i * chunk // heads + j
                top = jnp.where(here, m_ref[b, pl.ds(i * chunk + j * heads, heads), :], top)
                tot = jnp.where(here, total[j * heads : (j + 1) * heads], tot)
        lseb[b] = top * 128**-0.5 + jnp.log(tot)
        copies.append(pltpu.make_async_copy(lseb.at[b], lse_hbm.at[b], sem.at[b, CHUNKS]))
        copies[-1].start()
    for copy in copies:
        copy.wait()


def solution(mesh):
    def local(q, k, v, seg):
        batch, seq, heads, head = q.shape
        rows = seq * heads
        running = pl.pallas_call(
            gather_attend,
            out_shape=(pltpu.VMEM((batch, rows, 128), F32),) * 3 + (pltpu.VMEM((rows, 128), F32),),
            in_specs=[pl.BlockSpec(memory_space=pltpu.HBM)] * 4,
            out_specs=(pl.BlockSpec(memory_space=pltpu.VMEM),) * 4,
            scratch_shapes=[
                pltpu.VMEM((batch, rows, head), BF16),
                pltpu.VMEM((rows, 128), BF16),
                pltpu.VMEM((4, 2, batch, 2, seq, head), BF16),
                pltpu.VMEM((2, 2 * seq, 128), BF16),
                pltpu.VMEM((2, 2, 2 * seq, 128), BF16),
                pltpu.VMEM((8, batch, seq), jnp.int32),
                pltpu.SemaphoreType.DMA((3,)),
                pltpu.SemaphoreType.DMA((2,)),
                pltpu.SemaphoreType.DMA((4, 2)),
                pltpu.SemaphoreType.DMA((4,)),
                pltpu.SemaphoreType.REGULAR,
            ],
            compiler_params=pltpu.CompilerParams(collective_id=0, has_side_effects=True, vmem_limit_bytes=40 * 2**20),
        )(*[pltpu.with_memory_space_constraint(x, pltpu.HBM) for x in (q.reshape(batch, rows, head), k, v, seg)])
        out, lse = pl.pallas_call(
            normalise,
            out_shape=(jax.ShapeDtypeStruct((batch, rows, head), BF16), jax.ShapeDtypeStruct((batch, heads, seq), F32)),
            in_specs=[pl.BlockSpec(memory_space=pltpu.VMEM)] * 4,
            out_specs=(pl.BlockSpec(memory_space=pltpu.HBM),) * 2,
            scratch_shapes=[
                pltpu.VMEM((batch, rows, head), BF16),
                pltpu.VMEM((batch, heads, seq), F32),
                pltpu.SemaphoreType.DMA((batch, CHUNKS + 1)),
            ],
            compiler_params=pltpu.CompilerParams(vmem_limit_bytes=16 * 2**20),
        )(*running)
        return out.reshape(q.shape), lse.transpose(0, 2, 1)

    return jax.shard_map(
        local,
        mesh=mesh,
        in_specs=(P("dp", "cp", None, None), P("dp", "cp", None), P("dp", "cp", None), P("dp", "cp")),
        out_specs=(P("dp", "cp", None, None), P("dp", "cp", None)),
        check_vma=False,
    )
```

```python
import functools

import jax
import jax.numpy as jnp
import numpy as np
from jax import lax
from jax.experimental import pallas as pl
from jax.experimental.pallas import tpu as pltpu
from jax.sharding import PartitionSpec as P

MESH = pl.DeviceIdType.MESH
F32, BF16 = jnp.float32, jnp.bfloat16
HIDE = float(jnp.finfo(jnp.bfloat16).min)
LOG2E = float(np.log2(np.e))
NEXT, PREV, PART = 0, 1, 2
CHUNKS = 4
KV, SEG = 0, 1

IDS, LOADED, READY, OWN_IDS, OWN0, OWN1, NEAR_IDS, NEAR0, NEAR1, FAR0, FAR1, FAR2 = range(12)


def unit(c, b):
    return (KV, c, (1, 0), b)


def ids(c):
    return (SEG, c, (1, 0), 0)


def schedule():
    plan = {(c, q): {} for c in range(4) for q in range(2)}

    def put(c, q, point, *acts):
        plan[c, q].setdefault(point, []).extend(acts)

    def send(piece, *ways):
        return [("send", piece, w) for w in ways]

    def take(group, *ways):
        kind, c, qs, b = group
        return [("wait", group)] + [a for q in qs for a in send((kind, c, q, b), *ways)]

    for c in range(4):
        for q in range(2):
            on = [NEXT] if c < 3 else []
            put(c, q, IDS, *send((SEG, c, q, 0), *on, PART))
            put(c, q, OWN_IDS, *take((SEG, c, (1 - q,), 0)))
            for b in range(2):
                put(c, q, LOADED, *send((KV, c, q, b), *on, *([PREV] if (c, q, b) == (1, 0, 1) else []), PART))
                put(c, q, OWN0 + b, *take((KV, c, (1 - q,), b)))
            if c == 0:
                put(c, q, READY, *send((SEG, c, q, 0), PREV), *send((KV, c, q, 0), PREV), *send((KV, c, q, 1), PREV))
            if q == 0:
                if c:
                    put(c, q, NEAR_IDS, *take(ids(c - 1)))
                    put(c, q, NEAR0, *take(unit(c - 1, 0)))
                    put(c, q, NEAR1, *take(unit(c - 1, 1)))
                if c > 1:
                    put(c, q, NEAR1, *take(ids(0)))
                    put(c, q, FAR0, *take(unit(0, 0)))
                if c == 2:
                    put(c, q, FAR1, *take(unit(0, 1)))
                if c == 3:
                    put(c, q, NEAR1, *take(ids(1)))
                    put(c, q, FAR1, *take(unit(1, 0)))
                    put(c, q, FAR2, *take(unit(0, 1)), *take(unit(1, 1)))
    put(0, 1, OWN0, *take((KV, 1, (0,), 1), PREV))
    put(1, 1, OWN1, *take(ids(0), NEXT, PART), *take(unit(0, 0), NEXT, PART))
    put(1, 1, NEAR0, *take(unit(0, 1), NEXT, PART))
    put(2, 1, OWN1, *take(ids(1), NEXT, PART))
    put(2, 1, NEAR0, *take(unit(1, 0), NEXT, PART))
    put(2, 1, NEAR1, *take(unit(1, 1), PART), *send((KV, 1, 1, 1), NEXT), *take(ids(0), PART))
    put(2, 1, FAR0, *take(unit(0, 0), PART))
    put(2, 1, FAR1, *take(unit(0, 1), PART))
    put(3, 1, OWN1, *take(ids(2), PART))
    put(3, 1, NEAR0, *take(unit(2, 0), PART))
    put(3, 1, NEAR1, *take(unit(2, 1), PART), *take(ids(0), PART), *take(ids(1), PART))
    put(3, 1, FAR0, *take(unit(0, 0), PART))
    put(3, 1, FAR1, *take(unit(1, 0), PART), *take(unit(0, 1), PART), *take(unit(1, 1), PART))
    return plan


PLAN = schedule()


def attend(lhs, kk, vv, state, b, c2, first=False):
    m_ref, l_ref, acc_ref = state
    s = lax.dot_general(lhs, kk, (((1,), (1,)), ((), ())), preferred_element_type=F32)
    parts = [s[:, i : i + 128] for i in range(0, s.shape[1], 128)]
    m_new = jnp.broadcast_to(jnp.max(functools.reduce(jnp.maximum, parts), axis=1, keepdims=True), (s.shape[0], 128))
    if not first:
        m_prev = m_ref[b]
        m_new = jnp.maximum(m_prev, m_new)
        alpha = jnp.exp2((m_prev - m_new) * c2)
    parts = [jnp.exp2((x - m_new) * c2) for x in parts]
    m_ref[b] = m_new
    total = functools.reduce(jnp.add, parts)
    l_ref[b] = total if first else l_ref[b] * alpha + total
    p = jnp.concatenate([x.astype(BF16) for x in parts], axis=1)
    pv = lax.dot_general(p, vv, (((1,), (0,)), ((), ())), preferred_element_type=F32)
    acc_ref[b] = pv if first else acc_ref[b] * alpha + pv


def branch(index, leaves):
    keys = sorted(leaves)
    if len(keys) == 1:
        pl.when(index == keys[0])(leaves[keys[0]])
        return
    mid = keys[len(keys) // 2]
    pl.when(index < mid)(lambda: branch(index, {k: leaves[k] for k in keys if k < mid}))
    pl.when(index >= mid)(lambda: branch(index, {k: leaves[k] for k in keys if k >= mid}))


def gather_attend(q_hbm, k_hbm, v_hbm, seg_hbm, m_ref, l_ref, acc_ref, first_sum, qb, oh, kv, bias, far_bias, sg, ldsem, ssem, rsem, srsem, ready):
    me = lax.axis_index("cp")
    chip, core = me // 2, me % 2
    rows = qb.shape[1]
    heads = rows // 128
    c2 = 128**-0.5 * LOG2E

    def slot(item):
        kind, c, q, b = item
        return sg.at[c * 2 + q] if kind == SEG else kv.at[c, q, b]

    def wait(ref, sem):
        pltpu.make_async_copy(ref, ref, sem).wait()

    barrier = pltpu.get_barrier_semaphore()
    next_dev = lax.rem(chip + 1, 4) * 2 + 1
    prev_dev = lax.rem(chip + 3, 4) * 2 + 1
    part_dev = chip * 2 + 1 - core

    def greet(*devs):
        for dev in devs:
            pl.semaphore_signal(barrier, inc=1, device_id={"cp": dev}, device_id_type=MESH)

    greet(part_dev)
    pl.when((core == 1) & (chip > 0))(lambda: greet(prev_dev, prev_dev - 1))
    pl.when((core == 1) & (chip == 0))(lambda: greet(next_dev, next_dev - 1))
    pl.when(chip == 0)(lambda: greet(prev_dev))
    pltpu.make_async_copy(seg_hbm, sg.at[me], ldsem.at[0]).start()
    for i, src in enumerate((k_hbm, v_hbm)):
        pltpu.make_async_copy(src, kv.at[chip, core, :, i], ldsem.at[1]).start()
    q_load = pltpu.make_async_copy(q_hbm, qb, ldsem.at[2])
    q_load.start()

    for i, n in {0: 2, 1: 2, 2: 3, 3: 3, 4: 2, 5: 2, 6: 1, 7: 3}.items():
        pl.when(me == i)(lambda n=n: pl.semaphore_wait(barrier, n))

    @pl.when(me == 7)
    def _():
        for dev in (next_dev, next_dev - 1):
            pl.semaphore_signal(ready, inc=1, device_id={"cp": dev}, device_id_type=MESH)

    ways = (next_dev, prev_dev, part_dev)

    def run(actions):
        for act in actions:
            kind, c, q, b = act[1]
            arrival = srsem.at[c] if kind == SEG else rsem.at[c, b]
            if act[0] == "send":
                ref, left = slot(act[1]), ssem.at[kind]
                pltpu.make_async_remote_copy(src_ref=ref, dst_ref=ref, send_sem=left, recv_sem=arrival, device_id={"cp": ways[act[2]]}, device_id_type=MESH).start()
            elif kind == SEG:
                wait(sg.at[pl.ds(0, len(q))], arrival)
            else:
                wait(kv.at[c, pl.ds(0, len(q)), b], arrival)

    def at(point):
        acts = {c * 2 + q: points[point] for (c, q), points in PLAN.items() if point in points}
        branch(me, {i: lambda a=a: run(a) for i, a in acts.items()})

    wait(sg.at[me], ldsem.at[0])
    at(IDS)
    wait(kv.at[chip, core], ldsem.at[1])
    at(LOADED)

    @pl.when(chip == 0)
    def _():
        pl.semaphore_wait(ready, 1)
        at(READY)

    def fill(t, _):
        here = lax.broadcasted_iota(jnp.int32, (heads, 128), 1) == t
        oh[pl.ds(pl.multiple_of(t * heads, heads), heads), :] = jnp.where(here, 1.0, 0.0).astype(BF16)
        return 0

    lax.fori_loop(0, 128, fill, 0, unroll=16)
    q_load.wait()

    key = lax.broadcasted_iota(jnp.int32, (128, 128), 0)

    def hide(c, b, buf, local=False):
        seg_t = sg[me, pl.ds(b, 1), :]
        for half in range(2):
            seg_u = sg[c * 2 + half, pl.ds(b, 1), :]
            below = [jnp.broadcast_to(jnp.sum(jnp.where(seg_u < i, 1.0, 0.0), axis=1, keepdims=True), (1, 128)) for i in (1, 2)]
            smaller = jnp.where(seg_t == 0, 0.0, jnp.where(seg_t == 1, below[0], below[1])).astype(jnp.int32)
            seen = key >= smaller
            if local:
                t_pos = core * 128 + lax.broadcasted_iota(jnp.int32, (1, 128), 1)
                seen = seen & (key <= t_pos - half * 128)
            buf[pl.ds(half * 128, 128), :] = jnp.where(seen, 0.0, HIDE).astype(BF16)

    state = (m_ref, l_ref, acc_ref)

    def lhs(b):
        return jnp.concatenate([qb[b], oh[...]], axis=1)

    def keys(c, b, mask):
        kk = jnp.concatenate([kv[c, 0, b, 0], kv[c, 1, b, 0]], axis=0)
        return jnp.concatenate([kk, mask], axis=1), jnp.concatenate([kv[c, 0, b, 1], kv[c, 1, b, 1]], axis=0)

    def hide_far(c, b):
        hide(c, b, far_bias.at[b, c])

    at(OWN_IDS)
    for b in range(2):
        hide(chip, b, bias.at[b], local=True)
    for b in range(2):
        at(OWN0 + b)
        attend(lhs(b), *keys(chip, b, bias[b]), state, b, c2, first=True)

    def drain(steps):
        sent = [act[1][0] for acts in steps.values() for act in acts if act[0] == "send"]
        wait(acc_ref.at[0, pl.ds(0, sent.count(KV) * 128)], ssem.at[KV])
        wait(sg.at[pl.ds(0, sent.count(SEG))], ssem.at[SEG])

    def drained(core):
        branch(chip, {c: lambda steps=PLAN[c, core]: drain(steps) for c in range(4)})

    pl.when(core == 0)(lambda: drained(0))

    def sum_first():
        first_sum[...] = jnp.broadcast_to(jnp.sum(l_ref[0], axis=1, keepdims=True), (rows, 128))

    def one(c, b, mask):
        attend(lhs(b), *keys(c, b, mask), state, b, c2)

    @pl.when(chip > 0)
    def _():
        at(NEAR_IDS)
        for b in range(2):
            hide(chip - 1, b, bias.at[b])
        at(NEAR0)
        one(chip - 1, 0, bias[0])
        at(NEAR1)
        for c in range(2):
            for b in range(2):
                hide_far(c, b)
        one(chip - 1, 1, bias[1])

    @pl.when(chip > 1)
    def _():
        at(FAR0)
        one(0, 0, far_bias[0, 0])
        at(FAR1)
        unit1 = chip - 2
        one(unit1, 1 - unit1, far_bias[1 - unit1, unit1])

    @pl.when(chip > 2)
    def _():
        at(FAR2)
        sum_first()
        parts = [keys(c, 1, far_bias[1, c]) for c in range(2)]
        attend(lhs(1), *[jnp.concatenate(x, axis=0) for x in zip(*parts, strict=True)], state, 1, c2)

    pl.when(chip < 3)(sum_first)

    pl.when(core == 1)(lambda: drained(1))


def normalise(m_ref, l_ref, acc_ref, first_sum, o_hbm, lse_hbm, ob, lseb, sem):
    batch, rows, _ = acc_ref.shape
    heads = rows // 128
    chunk = rows // CHUNKS
    lane = lax.broadcasted_iota(jnp.int32, (heads, 128), 1)
    copies = []
    for b in range(batch):
        top = tot = jnp.zeros((heads, 128), F32)
        for i in range(CHUNKS):
            part = pl.ds(i * chunk, chunk)
            if b == 0:
                total = first_sum[part, :]
            else:
                total = jnp.broadcast_to(jnp.sum(l_ref[b, part, :], axis=1, keepdims=True), (chunk, 128))
            ob[b, part, :] = (acc_ref[b, part, :] * (1.0 / total)).astype(BF16)
            copies.append(pltpu.make_async_copy(ob.at[b, part], o_hbm.at[b, part], sem.at[b, i]))
            copies[-1].start()
            for j in range(chunk // heads):
                here = lane == i * chunk // heads + j
                top = jnp.where(here, m_ref[b, pl.ds(i * chunk + j * heads, heads), :], top)
                tot = jnp.where(here, total[j * heads : (j + 1) * heads], tot)
        lseb[b] = top * 128**-0.5 + jnp.log(tot)
        copies.append(pltpu.make_async_copy(lseb.at[b], lse_hbm.at[b], sem.at[b, CHUNKS]))
        copies[-1].start()
    for copy in copies:
        copy.wait()


def solution(mesh):
    def local(q, k, v, seg):
        batch, seq, heads, head = q.shape
        rows = seq * heads
        running = pl.pallas_call(
            gather_attend,
            out_shape=(pltpu.VMEM((batch, rows, 128), F32),) * 3 + (pltpu.VMEM((rows, 128), F32),),
            in_specs=[pl.BlockSpec(memory_space=pltpu.HBM)] * 4,
            out_specs=(pl.BlockSpec(memory_space=pltpu.VMEM),) * 4,
            scratch_shapes=[
                pltpu.VMEM((batch, rows, head), BF16),
                pltpu.VMEM((rows, 128), BF16),
                pltpu.VMEM((4, 2, batch, 2, seq, head), BF16),
                pltpu.VMEM((2, 2 * seq, 128), BF16),
                pltpu.VMEM((2, 2, 2 * seq, 128), BF16),
                pltpu.VMEM((8, batch, seq), jnp.int32),
                pltpu.SemaphoreType.DMA((3,)),
                pltpu.SemaphoreType.DMA((2,)),
                pltpu.SemaphoreType.DMA((4, 2)),
                pltpu.SemaphoreType.DMA((4,)),
                pltpu.SemaphoreType.REGULAR,
            ],
            compiler_params=pltpu.CompilerParams(collective_id=0, has_side_effects=True, vmem_limit_bytes=40 * 2**20),
        )(*[pltpu.with_memory_space_constraint(x, pltpu.HBM) for x in (q.reshape(batch, rows, head), k, v, seg)])
        out, lse = pl.pallas_call(
            normalise,
            out_shape=(jax.ShapeDtypeStruct((batch, rows, head), BF16), jax.ShapeDtypeStruct((batch, heads, seq), F32)),
            in_specs=[pl.BlockSpec(memory_space=pltpu.VMEM)] * 4,
            out_specs=(pl.BlockSpec(memory_space=pltpu.HBM),) * 2,
            scratch_shapes=[
                pltpu.VMEM((batch, rows, head), BF16),
                pltpu.VMEM((batch, heads, seq), F32),
                pltpu.SemaphoreType.DMA((batch, CHUNKS + 1)),
            ],
            compiler_params=pltpu.CompilerParams(vmem_limit_bytes=16 * 2**20),
        )(*running)
        return out.reshape(q.shape), lse.transpose(0, 2, 1)

    return jax.shard_map(
        local,
        mesh=mesh,
        in_specs=(P("dp", "cp", None, None), P("dp", "cp", None), P("dp", "cp", None), P("dp", "cp")),
        out_specs=(P("dp", "cp", None, None), P("dp", "cp", None)),
        check_vma=False,
    )
```
